256 devices in a mesh: pop: 64 (over z, y, core), tp: 4 (over x).
Axes of the slice: x: 4, y: 4, z: 8, core: 2. Of those that a mesh axis runs over, the one named last changes fastest.
Arguments:
- tokens: bfloat16 [65536, 5120], P('pop', 'tp'), may hold values from -6 to 6
- target: bfloat16 [65536, 5120], P('pop', 'tp'), may hold values from -6 to 6
- weight: bfloat16 [5120, 5120], P('pop', 'tp'), may hold values from -6 to 6
- factor_out: bfloat16 [256, 4, 5120], P('pop'), may hold values from -6 to 6
- factor_in: bfloat16 [256, 4, 5120], P('pop', None, 'tp'), may hold values from -6 to 6
Outputs:
- perturbed: bfloat16 [65536, 5120], P('pop', 'tp')
- new_weight: bfloat16 [5120, 5120], P('pop', 'tp')
The draws below stay inside these ranges and needn't reach their ends.
All inputs are finite; a program needn't handle non-finite values.
Results may differ from the reference program's by a relative error of at most 0.012.
Values may be sent and summed in bfloat16 or wider, within the bound.
A program may use at most 128 MiB of HBM per device.

```python
import math
import jax
import jax.numpy as jnp
from jax import lax

D_IN = 5120
D_OUT = 5120
R = 4
TOK_MEM = 256
MEMBERS = 256
TOKENS = 65536
N_TP = 4


def level_of(own_key, extent, shards, least, top_value):
    factor_of, own = 1.0, jax.random.fold_in(own_key, 6)
    for dim, parts in shards:
        draws = jnp.exp(jax.random.uniform(jax.random.fold_in(own, dim), (parts,), jnp.float32, least / len(shards), top_value / len(shards)))
        factor_of = factor_of * jnp.repeat(draws, extent[dim] // parts).reshape([-1 if axis == dim else 1 for axis in range(len(extent))])
    return factor_of


def gaussian(stream_key, extent, width, reach, split=(), held_as=jnp.bfloat16):
    array = jax.random.normal(stream_key, extent, jnp.float32) * width
    if len(split) > 0:
        array = level_of(stream_key, extent, split, -0.22, 0.18) * array
    return jnp.clip(array, min=-reach, max=reach).astype(held_as)


def setup_inputs(seed: int = 0) -> dict:
    splits = jax.random.split(jax.random.key(seed), 6)
    tokens = gaussian(splits[0], (TOKENS, D_IN), 1.0, 6.0, ((0, 64), (1, 4)))
    target = gaussian(splits[1], (TOKENS, D_OUT), 1.0, 6.0, ((0, 64), (1, 4)))
    weight = gaussian(splits[2], (D_OUT, D_IN), 1.0, 6.0, ((0, 64), (1, 4)))
    factor_out = gaussian(splits[3], (MEMBERS, R, D_OUT), 1.0, 6.0, ((0, 64),))
    factor_in = gaussian(splits[4], (MEMBERS, R, D_IN), 1.0, 6.0, ((0, 64), (2, 4)))
    return dict(tokens=tokens, target=target, weight=weight, factor_out=factor_out, factor_in=factor_in)


noise_scale = 0.25
step_scale = 10.0

def reference(tokens, target, weight, factor_out, factor_in):
    shard_width = D_IN // N_TP
    token_sets = tokens.reshape(MEMBERS, TOK_MEM, D_IN)
    target_sets = target.reshape(MEMBERS, TOK_MEM, D_OUT)

    def member(member_parts):
        inputs, wanted, outer, inner = member_parts
        total = jnp.zeros((TOK_MEM, D_OUT), jnp.float32)
        for block in range(N_TP):
            lower = block * shard_width
            upper = lower + shard_width
            partial_value = jnp.dot(inputs[:, lower:upper], weight[:, lower:upper].T, preferred_element_type=jnp.float32) / math.sqrt(D_IN)
            total = total + lax.optimization_barrier(partial_value.astype(jnp.bfloat16)).astype(jnp.float32)
        codes_all = jnp.dot(inputs.astype(jnp.float32), inner.astype(jnp.float32).T, precision=lax.Precision.HIGHEST)
        low_rank = jnp.dot(codes_all, outer.astype(jnp.float32), precision=lax.Precision.HIGHEST) * (noise_scale / math.sqrt(R * D_IN))
        output_full = total + low_rank
        fitness_one = jnp.sum(output_full * wanted.astype(jnp.float32)) / (TOK_MEM * math.sqrt(D_OUT))
        return (output_full.astype(jnp.bfloat16), fitness_one)
    outputs, fitness = lax.map(member, (token_sets, target_sets, factor_out, factor_in))
    centered = fitness - jnp.mean(fitness)
    scaled = (centered[:, None, None] * factor_out.astype(jnp.float32)).astype(jnp.bfloat16)
    delta = jnp.dot(scaled.reshape(MEMBERS * R, D_OUT).T, factor_in.reshape(MEMBERS * R, D_IN), preferred_element_type=jnp.float32)
    updated = (weight.astype(jnp.float32) + step_scale / math.sqrt(MEMBERS * R) * delta).astype(jnp.bfloat16)
    return (outputs.reshape(TOKENS, D_OUT), updated)
```

```python
import math

import jax
import jax.numpy as jnp
from jax import lax
from jax.experimental import pallas as pl
from jax.experimental.pallas import tpu as pltpu

noise_scale = 0.25
step_scale = 10.0

F32 = jnp.float32
BF16 = jnp.bfloat16
NX, NY, NZ = 4, 4, 8
NSTEP = 8


def kernel(tok, tgt, wt, fo, fin, out, neww,
           T, W, FIN, TG, WL, ACC, S32, FOS, FO2, FO3, FP, FX, FY, FZ,
           loc, tr, tl, tf, wa, wz, yu, yd, fu, fd, d2, fxs, fny, fnu, fnd, fnc,
           foy, foz, gx, gy, gz,
           s_tok, s_tf, s_wa, s_w, s_d2, s_fx, s_fny, s_fnz, s_fnc, s_foy, s_foz, s_gx, s_gy, s_gz):
    p = lax.axis_index("pop")
    x = lax.axis_index("tp")
    z = p // 8
    e = p % 8
    y = e // 2
    c = e % 2
    rows, kw = tok.shape
    mem = rows // 4
    sr = wt.shape[0]
    half = 8 * sr
    rank16 = 16
    width_in = kw * NX
    width_out = width_in

    def pop_of(zz, ee):
        return lax.rem(zz, 8) * 8 + lax.rem(ee, 8)

    def rc(src, dst, ss, rs, pop, tp):
        return pltpu.make_async_remote_copy(
            src_ref=src, dst_ref=dst, send_sem=ss, recv_sem=rs,
            device_id={"pop": pop, "tp": tp}, device_id_type=pl.DeviceIdType.MESH)

    xr = lax.rem(x + 1, 4)
    xl = lax.rem(x + 3, 4)
    zu = pop_of(z + 1, e)
    zd = pop_of(z + 7, e)
    yup = z * 8 + lax.rem(y + 1, 4) * 2 + c
    ydn = z * 8 + lax.rem(y + 3, 4) * 2 + c
    sib = z * 8 + y * 2 + (1 - c)

    l_wl = pltpu.make_async_copy(wt, WL, loc.at[0])
    l_t0 = pltpu.make_async_copy(tok, T.at[0], loc.at[1])
    l_tg = pltpu.make_async_copy(tgt, TG, loc.at[2])
    l_wl.start()
    l_t0.start()
    l_tg.start()

    bar = pltpu.get_barrier_semaphore()
    for k in range(1, 4):
        pl.semaphore_signal(bar, inc=1, device_id={"pop": p, "tp": lax.rem(x + k, 4)},
                            device_id_type=pl.DeviceIdType.MESH)
    for k in range(1, 8):
        pl.semaphore_signal(bar, inc=1, device_id={"pop": z * 8 + lax.rem(e + k, 8), "tp": x},
                            device_id_type=pl.DeviceIdType.MESH)
        pl.semaphore_signal(bar, inc=1, device_id={"pop": pop_of(z + k, e), "tp": x},
                            device_id_type=pl.DeviceIdType.MESH)
    pl.semaphore_wait(bar, 17)

    zt = z // 2
    r_own = lax.rem(z, 2)
    off = lax.rem(x - zt + 4, 4)
    slot = off + off // 2 - 2 * (off // 3)
    shard = pl.ds(pl.multiple_of(e * sr, 16), sr)
    send_a = rc(wt, W.at[slot, r_own, shard], s_wa, wa.at[slot], p, zt)
    copy_a = pltpu.make_async_copy(wt, W.at[0, r_own, shard], loc.at[3])

    @pl.when(off == 0)
    def _():
        copy_a.start()

    @pl.when(off != 0)
    def _():
        send_a.start()

    for i in range(4):
        S32[4 * i:4 * i + 4, 0:kw] = fin[i].astype(F32)
    fin16 = S32[:, 0:kw].astype(BF16)
    FP[...] = fin16
    FIN[z, y, c] = fin16
    W[0, 0, half:half + rank16] = fin16
    xslot = {1: 2, 2: 3, 3: 1}
    for k in range(1, 4):
        rc(FP, W.at[xslot[k], 0, half:half + rank16], s_fx.at[k], fxs.at[k], p, lax.rem(x + k, 4)).start()

    def chunk(m):
        return pl.ds(m * mem, mem)

    def tok_right(m):
        return rc(tok.at[chunk(m)], T.at[2, chunk(m)], s_tok.at[0, m], tr.at[m], p, xr)

    def tok_left(m):
        return rc(tok.at[chunk(m)], T.at[1, chunk(m)], s_tok.at[1, m], tl.at[m], p, xl)

    def tok_fwd(m):
        if m % 2 == 0:
            return rc(T.at[2, chunk(m)], T.at[3, chunk(m)], s_tf.at[m], tf.at[m], p, xr)
        return rc(T.at[1, chunk(m)], T.at[3, chunk(m)], s_tf.at[m], tf.at[m], p, xl)

    for m in range(4):
        tok_right(m).start()
        tok_left(m).start()

    def fin_y(k):
        return rc(FP, FIN.at[z, y, c], s_fny.at[k], fny.at[k],
                  z * 8 + lax.rem(y + k, 4) * 2 + c, x)

    def fin_y_in(k):
        return rc(FP, FIN.at[z, lax.rem(y + 4 - k, 4), c], s_fny.at[k], fny.at[k], p, x)

    for k in range(1, 4):
        fin_y(k).start()

    for i in range(4):
        S32[4 * i:4 * i + 4, :] = fo[i].astype(F32)
    grp = 8 * sr
    sel_row = lax.broadcasted_iota(jnp.int32, (grp, 1024), 0)
    sel_col = lax.broadcasted_iota(jnp.int32, (grp, 1024), 1)
    lane = lax.rem(sel_col, 128)
    want = (sel_col // 128) * sr + lane
    sel = jnp.where((sel_row == want) & (lane < sr), 1.0, 0.0).astype(BF16)
    for g in range(8):
        cut = jnp.dot(S32[:, g * grp:(g + 1) * grp].astype(BF16), sel,
                      preferred_element_type=F32).astype(BF16)
        for d in range(8):
            FOS[d, g] = cut[:, d * 128:(d + 1) * 128]
    FO2[e] = FOS[e]

    def fo_y(k):
        ee = lax.rem(e + k, 8)
        return rc(FOS.at[ee], FO2.at[e], s_foy.at[k], foy.at[k], z * 8 + ee, x)

    def fo_y_in(k):
        return rc(FOS.at[0], FO2.at[lax.rem(e + 8 - k, 8)], s_foy.at[k], foy.at[k], p, x)

    for k in range(1, 8):
        fo_y(k).start()

    def fo_z(k):
        zz = lax.rem(z + k, 8)
        return rc(FO2.at[:, zz], FO3.at[z], s_foz.at[k], foz.at[k], zz * 8 + e, x)

    def fo_z_in(k):
        return rc(FO2.at[:, 0], FO3.at[lax.rem(z + 8 - k, 8)], s_foz.at[k], foz.at[k], p, x)

    l_wl.wait()
    l_t0.wait()
    l_tg.wait()

    rz = lax.rem(z + 8 - 2 * x, 8)

    def shard_at(s, yy, cols=None):
        q = lax.rem(yy, 4) * 2 + c
        rws = pl.ds(pl.multiple_of(q * sr, 16), sr)
        ref = W.at[s // 2, s % 2, rws]
        if cols is not None:
            ref = W.at[s // 2, s % 2, rws, pl.ds(cols * (kw // 2), kw // 2)]
        return ref

    def z_in(s):
        return rc(shard_at(s, y), shard_at(s, y), s_w.at[0, s], wz.at[s], p, x)

    def z_up(s):
        return rc(shard_at(s, y), shard_at(s, y), s_w.at[0, s], wz.at[s], zu, x)

    def z_dn(s):
        return rc(shard_at(s, y), shard_at(s, y), s_w.at[1, s], wz.at[s], zd, x)

    def y_up(s):
        return rc(shard_at(s, y), shard_at(s, y), s_w.at[2, s], yu.at[s], yup, x)

    def y_up_in(s):
        return rc(shard_at(s, y + 3), shard_at(s, y + 3), s_w.at[2, s], yu.at[s], p, x)

    def y_dn(s):
        return rc(shard_at(s, y), shard_at(s, y), s_w.at[3, s], yd.at[s], ydn, x)

    def y_dn_in(s):
        return rc(shard_at(s, y + 1), shard_at(s, y + 1), s_w.at[3, s], yd.at[s], p, x)

    def f_up(s):
        return rc(shard_at(s, y + 3, 0), shard_at(s, y + 3, 0), s_w.at[4, s], fu.at[s], yup, x)

    def f_up_in(s):
        return rc(shard_at(s, y + 2, 0), shard_at(s, y + 2, 0), s_w.at[4, s], fu.at[s], p, x)

    def f_dn(s):
        return rc(shard_at(s, y + 1, 1), shard_at(s, y + 1, 1), s_w.at[5, s], fd.at[s], ydn, x)

    def f_dn_in(s):
        return rc(shard_at(s, y + 2, 1), shard_at(s, y + 2, 1), s_w.at[5, s], fd.at[s], p, x)

    def pass_on(s, k):
        return rc(shard_at(s, y + k), shard_at(s, y + k), s_d2.at[k, s], d2.at[s], sib, x)

    def sib_in(s):
        whole = W.at[s // 2, s % 2, 0:4 * sr]
        return rc(whole, whole, s_d2.at[0, s], d2.at[s], p, x)

    def up_pred(s):
        if s % 2 == 0:
            return rz <= 3
        return (rz >= 1) & (rz <= 3)

    def dn_pred(s):
        if s % 2 == 0:
            return (rz == 0) | (rz >= 6)
        return (rz <= 1) | (rz >= 6)

    def stage_a(s):
        j, r = s // 2, s % 2

        @pl.when(rz == r)
        def _():
            if j == 0:
                copy_a.wait()
            else:
                rc(shard_at(s, y), shard_at(s, y), s_wa, wa.at[j], p, x).wait_recv()

        @pl.when(rz != r)
        def _():
            z_in(s).wait_recv()

        @pl.when(up_pred(s))
        def _():
            z_up(s).start()

        @pl.when(dn_pred(s))
        def _():
            z_dn(s).start()

        y_up(s).start()
        y_dn(s).start()
        pass_on(s, 0).start()

    def stage_b(s):
        y_up_in(s).wait_recv()
        f_up(s).start()
        pass_on(s, 3).start()
        y_dn_in(s).wait_recv()
        f_dn(s).start()
        pass_on(s, 1).start()

    def stage_c(s):
        f_up_in(s).wait_recv()
        f_dn_in(s).wait_recv()
        pass_on(s, 2).start()

    def compute(s):
        j, r = s // 2, s % 2
        sib_in(s).wait_recv()
        blk = rows // 2

        def body(i, _):
            rws = pl.ds(pl.multiple_of(i * blk, blk), blk)
            prod = lax.dot_general(T[j, rws], W[j, r], (((1,), (1,)), ((), ())),
                                   preferred_element_type=F32)
            if j == 0:
                ACC[r, rws] = prod
            else:
                ACC[r, rws] += prod
            return 0

        lax.fori_loop(0, 2, body, 0)

    def fin_block(zz, lo, n):
        return FIN.at[lax.rem(zz, 8), lo:lo + n, c]

    def fin_up(h):
        lo, n = (0, 4) if h < 4 else (0, 2)
        ref = fin_block(z + 9 - h, lo, n)
        return rc(ref, ref, s_fnz.at[0, h], fnu.at[h], zu, x)

    def fin_up_in(h):
        lo, n = (0, 4) if h < 4 else (0, 2)
        ref = fin_block(z + 8 - h, lo, n)
        return rc(ref, ref, s_fnz.at[0, h], fnu.at[h], p, x)

    def fin_dn(h):
        lo, n = (0, 4) if h < 4 else (2, 2)
        ref = fin_block(z + h - 1, lo, n)
        return rc(ref, ref, s_fnz.at[1, h], fnd.at[h], zd, x)

    def fin_dn_in(h):
        lo, n = (0, 4) if h < 4 else (2, 2)
        ref = fin_block(z + h, lo, n)
        return rc(ref, ref, s_fnz.at[1, h], fnd.at[h], p, x)

    def fin_sib():
        ref = FIN.at[:, :, c]
        return rc(ref, ref, s_fnc, fnc, sib, x)

    def fin_sib_in():
        ref = FIN.at[:, :, 1 - c]
        return rc(ref, ref, s_fnc, fnc, p, x)

    base_factor = 1.0 / math.sqrt(width_in)
    low_factor = noise_scale / math.sqrt(4 * width_in)
    lanes = lax.broadcasted_iota(jnp.int32, (8, 128), 1)
    sub = lax.broadcasted_iota(jnp.int32, (8, 128), 0)

    def epilogue(r):
        cols = slice(r * half, (r + 1) * half)
        first = pl.multiple_of(x * kw + r * half, 128)
        outer = S32[:, pl.ds(first, half)].astype(BF16)
        for m in range(4):
            rws = slice(m * mem, (m + 1) * mem)
            codes = ACC[0, rws, half:half + rank16]
            col = lax.broadcasted_iota(jnp.int32, (mem, rank16), 1)
            codes = jnp.where(col // 4 == m, codes, 0.0)
            hi = codes.astype(BF16)
            lo = (codes - hi.astype(F32)).astype(BF16)
            low = jnp.dot(hi, outer, preferred_element_type=F32) + jnp.dot(
                lo, outer, preferred_element_type=F32)
            full = ACC[r, rws, 0:half] * base_factor + low * low_factor
            out[rws, cols] = full.astype(BF16)
            part = jnp.sum(full * TG[rws, cols].astype(F32)) / (mem * math.sqrt(width_out))
            FX[0] += jnp.where((sub == e) & (lanes == m), part, 0.0)

    FX[0] = jnp.zeros((8, 128), F32)

    work = {3: (0,), 4: (1,), 7: (2, 3), 8: (4, 5), 9: (6,), 10: (7,)}
    for s in range(11):
        if s < 8:
            stage_a(s)
        if 1 <= s <= 8:
            stage_b(s - 1)
        if 2 <= s <= 9:
            stage_c(s - 2)
        if s == 2:
            tr_in(tok_right, 0)
            tok_fwd(0).start()
        if s == 3:
            for k in range(1, 4):
                fin_y_in(k).wait_recv()
            for k in range(1, 4):
                rc(FP, W.at[xslot[k], 0, half:half + rank16], s_fx.at[k], fxs.at[k], p, x).wait_recv()
        if 4 <= s <= 7:
            h = s - 3
            if h > 1:
                fin_up_in(h - 1).wait_recv()
                fin_dn_in(h - 1).wait_recv()
            fin_up(h).start()
            fin_dn(h).start()
        if s == 4:
            tr_in(tok_left, 1)
            tok_fwd(1).start()
        if s == 6:
            tr_in(tok_right, 2)
            tok_fwd(2).start()
        if s == 7:
            for m in (0, 2, 3):
                tr_in(tok_left, m)
            tok_fwd(3).start()
        if s == 8:
            for k in range(1, 8):
                fo_y_in(k).wait_recv()
            for k in range(1, 8):
                fo_z(k).start()
            FO3[z] = FO2[:, z]
            for m in (1, 3):
                tr_in(tok_right, m)
        if s == 9:
            fin_up_in(4).wait_recv()
            fin_dn_in(4).wait_recv()
            fin_sib().start()
            for m in range(4):
                tok_fwd(m).wait_recv()
        for k in work.get(s, ()):
            compute(k)
        if s == 9:
            epilogue(0)
    epilogue(1)

    def g_x(k):
        return rc(FX.at[0], FX.at[k], s_gx.at[k], gx.at[k], p, lax.rem(x + k, 4))

    for k in range(1, 4):
        g_x(k).start()
    for k in range(1, 4):
        g_x(k).wait_recv()
    FY[0] = FX[0] + FX[1] + FX[2] + FX[3]

    def g_y(k):
        return rc(FY.at[0], FY.at[k], s_gy.at[k], gy.at[k], z * 8 + lax.rem(e + k, 8), x)

    for k in range(1, 8):
        g_y(k).start()
    for k in range(1, 8):
        g_y(k).wait_recv()
    plane = FY[0]
    for k in range(1, 8):
        plane = plane + FY[k]
    FP32 = plane
    FZ[z] = FP32

    def g_z(k):
        return rc(FZ.at[z], FZ.at[z], s_gz.at[k], gz.at[k], pop_of(z + k, e), x)

    def g_z_in(k):
        ref = FZ.at[lax.rem(z + 8 - k, 8)]
        return rc(ref, ref, s_gz.at[k], gz.at[k], p, x)

    for k in range(1, 8):
        g_z(k).start()
    for k in range(1, 8):
        fo_z_in(k).wait_recv()
    fin_sib_in().wait_recv()
    for k in range(1, 8):
        g_z_in(k).wait_recv()

    grid = FZ[...].reshape(64, 128)
    mean = jnp.sum(grid) / 256.0
    wide = jnp.broadcast_to(grid[:, None, :], (64, 16, 128)).reshape(1024, 128)
    rr = lax.broadcasted_iota(jnp.int32, (1024, 128), 0)
    cc = lax.broadcasted_iota(jnp.int32, (1024, 128), 1)
    mine = jnp.where(cc == lax.rem(rr, 16) // 4, wide, 0.0)
    centered = jnp.sum(mine, axis=1, keepdims=True) - mean
    scaled = (centered * FO3[...].reshape(1024, 128).astype(F32)).astype(BF16)
    delta = lax.dot_general(scaled, FIN[...].reshape(1024, kw), (((0,), (0,)), ((), ())),
                            preferred_element_type=F32)
    neww[...] = (WL[...].astype(F32) + step_scale / math.sqrt(1024.0) * delta[0:sr]).astype(BF16)

    @pl.when(off != 0)
    def _():
        send_a.wait_send()

    for k in range(1, 4):
        rc(FP, W.at[xslot[k], 0, half:half + rank16], s_fx.at[k], fxs.at[k], p, x).wait_send()
        fin_y(k).wait_send()
        g_x(k).wait_send()
    for m in range(4):
        tok_right(m).wait_send()
        tok_left(m).wait_send()
        tok_fwd(m).wait_send()
    for s in range(NSTEP):
        @pl.when(up_pred(s))
        def _():
            z_up(s).wait_send()

        @pl.when(dn_pred(s))
        def _():
            z_dn(s).wait_send()

        y_up(s).wait_send()
        y_dn(s).wait_send()
        f_up(s).wait_send()
        f_dn(s).wait_send()
        for k in range(4):
            pass_on(s, k).wait_send()
    for h in range(1, 5):
        fin_up(h).wait_send()
        fin_dn(h).wait_send()
    fin_sib().wait_send()
    for k in range(1, 8):
        fo_y(k).wait_send()
        fo_z(k).wait_send()
        g_y(k).wait_send()
        g_z(k).wait_send()


def tr_in(make, m):
    make(m).wait_recv()


def local(tokens, target, weight, factor_out, factor_in):
    rows, kw = tokens.shape
    sr = weight.shape[0]
    half = 8 * sr
    width = factor_out.shape[2]
    any_spec = pl.BlockSpec(memory_space=pl.ANY)
    vm = pl.BlockSpec(memory_space=pltpu.VMEM)
    D = pltpu.SemaphoreType.DMA
    scratch = [
        pltpu.VMEM((4, rows, kw), BF16),
        pltpu.VMEM((4, 2, half + 16, kw), BF16),
        pltpu.VMEM((8, 4, 2, 16, kw), BF16),
        pltpu.VMEM((rows, kw), BF16),
        pltpu.VMEM((sr, kw), BF16),
        pltpu.VMEM((2, rows, half + 16), F32),
        pltpu.VMEM((16, width), F32),
        pltpu.VMEM((8, 8, 16, 128), BF16),
        pltpu.VMEM((8, 8, 16, 128), BF16),
        pltpu.VMEM((8, 8, 16, 128), BF16),
        pltpu.VMEM((16, kw), BF16),
        pltpu.VMEM((4, 8, 128), F32),
        pltpu.VMEM((8, 8, 128), F32),
        pltpu.VMEM((8, 8, 128), F32),
        D((4,)), D((4,)), D((4,)), D((4,)), D((4,)), D((8,)), D((8,)), D((8,)), D((8,)), D((8,)), D((8,)),
        D((4,)), D((4,)), D((5,)), D((5,)), D(()), D((8,)), D((8,)), D((4,)), D((8,)), D((8,)),
        D((2, 4)), D((4,)), D(()), D((6, 8)), D((4, 8)), D((4,)), D((4,)), D((2, 5)), D(()),
        D((8,)), D((8,)), D((4,)), D((8,)), D((8,)),
    ]
    return pl.pallas_call(
        kernel,
        out_shape=(jax.ShapeDtypeStruct((rows, kw), BF16), jax.ShapeDtypeStruct((sr, kw), BF16)),
        in_specs=[any_spec, any_spec, any_spec, vm, vm],
        out_specs=(vm, vm),
        scratch_shapes=scratch,
        compiler_params=pltpu.CompilerParams(
            collective_id=0, has_side_effects=True, vmem_limit_bytes=62 * 1024 * 1024),
    )(tokens, target, weight, factor_out, factor_in)


def solution(mesh):
    from jax.sharding import PartitionSpec as P

    in_specs = (
        P("pop", "tp"),
        P("pop", "tp"),
        P("pop", "tp"),
        P("pop", None, None),
        P("pop", None, "tp"),
    )
    out_specs = (P("pop", "tp"), P("pop", "tp"))
    return jax.shard_map(local, mesh=mesh, in_specs=in_specs, out_specs=out_specs, check_vma=False)
```

```python
import math

import jax
import jax.numpy as jnp
from jax import lax
from jax.experimental import pallas as pl
from jax.experimental.pallas import tpu as pltpu

noise_scale = 0.25
step_scale = 10.0

F32 = jnp.float32
BF16 = jnp.bfloat16
NX, NY, NZ = 4, 4, 8
NSTEP = 8


def kernel(tok, tgt, wt, fo_hbm, fin_hbm, out, neww,
           fo, fin, T, W, FIN, TG, WL, ACC, S32, FOS, FO2, FO3, FP, FX, FY, FZ,
           loc, tr, tl, tf, wa, wz, yu, yd, fu, fd, d2, fxs, fny, fnu, fnd, fnc,
           foy, foz, gx, gy, gz,
           s_tok, s_tf, s_wa, s_w, s_d2, s_fx, s_fny, s_fnz, s_fnc, s_foy, s_foz, s_gx, s_gy, s_gz):
    p = lax.axis_index("pop")
    x = lax.axis_index("tp")
    z = p // 8
    e = p % 8
    y = e // 2
    c = e % 2
    rows, kw = tok.shape
    mem = rows // 4
    sr = wt.shape[0]
    half = 8 * sr
    rank16 = 16
    width_in = kw * NX
    width_out = width_in

    def pop_of(zz, ee):
        return lax.rem(zz, 8) * 8 + lax.rem(ee, 8)

    def rc(src, dst, ss, rs, pop, tp):
        return pltpu.make_async_remote_copy(
            src_ref=src, dst_ref=dst, send_sem=ss, recv_sem=rs,
            device_id={"pop": pop, "tp": tp}, device_id_type=pl.DeviceIdType.MESH)

    xr = lax.rem(x + 1, 4)
    xl = lax.rem(x + 3, 4)
    zu = pop_of(z + 1, e)
    zd = pop_of(z + 7, e)
    yup = z * 8 + lax.rem(y + 1, 4) * 2 + c
    ydn = z * 8 + lax.rem(y + 3, 4) * 2 + c
    sib = z * 8 + y * 2 + (1 - c)

    l_wl = pltpu.make_async_copy(wt, WL, loc.at[0])
    l_t0 = pltpu.make_async_copy(tok, T.at[0], loc.at[1])
    l_tg = pltpu.make_async_copy(tgt, TG, loc.at[2])
    l_fi = pltpu.make_async_copy(fin_hbm, fin, loc.at[4])
    l_fo = pltpu.make_async_copy(fo_hbm, fo, loc.at[5])
    l_fi.start()
    l_fo.start()
    l_wl.start()
    l_t0.start()
    l_tg.start()

    bar = pltpu.get_barrier_semaphore()
    for k in range(1, 4):
        pl.semaphore_signal(bar, inc=1, device_id={"pop": p, "tp": lax.rem(x + k, 4)},
                            device_id_type=pl.DeviceIdType.MESH)
    for k in range(1, 8):
        pl.semaphore_signal(bar, inc=1, device_id={"pop": z * 8 + lax.rem(e + k, 8), "tp": x},
                            device_id_type=pl.DeviceIdType.MESH)
        pl.semaphore_signal(bar, inc=1, device_id={"pop": pop_of(z + k, e), "tp": x},
                            device_id_type=pl.DeviceIdType.MESH)
    l_fi.wait()
    for i in range(4):
        S32[4 * i:4 * i + 4, 0:kw] = fin[i].astype(F32)
    fin16 = S32[:, 0:kw].astype(BF16)
    FP[...] = fin16
    FIN[z, y, c] = fin16
    W[0, 0, half:half + rank16] = fin16
    l_fo.wait()
    for i in range(4):
        S32[4 * i:4 * i + 4, :] = fo[i].astype(F32)
    grp = 8 * sr
    sel_row = lax.broadcasted_iota(jnp.int32, (grp, 1024), 0)
    sel_col = lax.broadcasted_iota(jnp.int32, (grp, 1024), 1)
    lane = lax.rem(sel_col, 128)
    want = (sel_col // 128) * sr + lane
    sel = jnp.where((sel_row == want) & (lane < sr), 1.0, 0.0).astype(BF16)
    for g in range(8):
        cut = jnp.dot(S32[:, g * grp:(g + 1) * grp].astype(BF16), sel,
                      preferred_element_type=F32).astype(BF16)
        for d in range(8):
            FOS[d, g] = cut[:, d * 128:(d + 1) * 128]
    FO2[e] = FOS[e]

    pl.semaphore_wait(bar, 17)

    zt = z // 2
    r_own = lax.rem(z, 2)
    off = lax.rem(x - zt + 4, 4)
    slot = off + off // 2 - 2 * (off // 3)
    shard = pl.ds(pl.multiple_of(e * sr, 16), sr)
    send_a = rc(wt, W.at[slot, r_own, shard], s_wa, wa.at[slot], p, zt)
    copy_a = pltpu.make_async_copy(wt, W.at[0, r_own, shard], loc.at[3])

    @pl.when(off == 0)
    def _():
        copy_a.start()

    @pl.when(off != 0)
    def _():
        send_a.start()

    xslot = {1: 2, 2: 3, 3: 1}
    for k in range(1, 4):
        rc(FP, W.at[xslot[k], 0, half:half + rank16], s_fx.at[k], fxs.at[k], p, lax.rem(x + k, 4)).start()

    def chunk(m):
        return pl.ds(m * mem, mem)

    def tok_right(m):
        return rc(tok.at[chunk(m)], T.at[2, chunk(m)], s_tok.at[0, m], tr.at[m], p, xr)

    def tok_left(m):
        return rc(tok.at[chunk(m)], T.at[1, chunk(m)], s_tok.at[1, m], tl.at[m], p, xl)

    def tok_fwd(m):
        if m % 2 == 0:
            return rc(T.at[2, chunk(m)], T.at[3, chunk(m)], s_tf.at[m], tf.at[m], p, xr)
        return rc(T.at[1, chunk(m)], T.at[3, chunk(m)], s_tf.at[m], tf.at[m], p, xl)

    for m in (0, 2, 1, 3):
        tok_right(m).start()
        tok_left(3 - m).start()

    def fin_y(k):
        return rc(FP, FIN.at[z, y, c], s_fny.at[k], fny.at[k],
                  z * 8 + lax.rem(y + k, 4) * 2 + c, x)

    def fin_y_in(k):
        return rc(FP, FIN.at[z, lax.rem(y + 4 - k, 4), c], s_fny.at[k], fny.at[k], p, x)

    for k in range(1, 4):
        fin_y(k).start()

    def fo_y(k):
        ee = lax.rem(e + k, 8)
        return rc(FOS.at[ee], FO2.at[e], s_foy.at[k], foy.at[k], z * 8 + ee, x)

    def fo_y_in(k):
        return rc(FOS.at[0], FO2.at[lax.rem(e + 8 - k, 8)], s_foy.at[k], foy.at[k], p, x)

    for k in range(1, 8):
        fo_y(k).start()

    def fo_z(k):
        zz = lax.rem(z + k, 8)
        return rc(FO2.at[:, zz], FO3.at[z], s_foz.at[k], foz.at[k], zz * 8 + e, x)

    def fo_z_in(k):
        return rc(FO2.at[:, 0], FO3.at[lax.rem(z + 8 - k, 8)], s_foz.at[k], foz.at[k], p, x)

    l_wl.wait()
    l_t0.wait()
    l_tg.wait()

    rz = lax.rem(z + 8 - 2 * x, 8)

    def shard_at(s, yy, cols=None):
        q = lax.rem(yy, 4) * 2 + c
        rws = pl.ds(pl.multiple_of(q * sr, 16), sr)
        ref = W.at[s // 2, s % 2, rws]
        if cols is not None:
            ref = W.at[s // 2, s % 2, rws, pl.ds(cols * (kw // 2), kw // 2)]
        return ref

    def z_in(s):
        return rc(shard_at(s, y), shard_at(s, y), s_w.at[0, s], wz.at[s], p, x)

    def z_up(s):
        return rc(shard_at(s, y), shard_at(s, y), s_w.at[0, s], wz.at[s], zu, x)

    def z_dn(s):
        return rc(shard_at(s, y), shard_at(s, y), s_w.at[1, s], wz.at[s], zd, x)

    def y_up(s):
        return rc(shard_at(s, y), shard_at(s, y), s_w.at[2, s], yu.at[s], yup, x)

    def y_up_in(s):
        return rc(shard_at(s, y + 3), shard_at(s, y + 3), s_w.at[2, s], yu.at[s], p, x)

    def y_dn(s):
        return rc(shard_at(s, y), shard_at(s, y), s_w.at[3, s], yd.at[s], ydn, x)

    def y_dn_in(s):
        return rc(shard_at(s, y + 1), shard_at(s, y + 1), s_w.at[3, s], yd.at[s], p, x)

    def f_up(s):
        return rc(shard_at(s, y + 3, 0), shard_at(s, y + 3, 0), s_w.at[4, s], fu.at[s], yup, x)

    def f_up_in(s):
        return rc(shard_at(s, y + 2, 0), shard_at(s, y + 2, 0), s_w.at[4, s], fu.at[s], p, x)

    def f_dn(s):
        return rc(shard_at(s, y + 1, 1), shard_at(s, y + 1, 1), s_w.at[5, s], fd.at[s], ydn, x)

    def f_dn_in(s):
        return rc(shard_at(s, y + 2, 1), shard_at(s, y + 2, 1), s_w.at[5, s], fd.at[s], p, x)

    def pass_on(s, k):
        return rc(shard_at(s, y + k), shard_at(s, y + k), s_d2.at[k, s], d2.at[s], sib, x)

    def sib_in(s):
        whole = W.at[s // 2, s % 2, 0:4 * sr]
        return rc(whole, whole, s_d2.at[0, s], d2.at[s], p, x)

    def up_pred(s):
        if s % 2 == 0:
            return rz <= 3
        return (rz >= 1) & (rz <= 3)

    def dn_pred(s):
        if s % 2 == 0:
            return (rz == 0) | (rz >= 6)
        return (rz <= 1) | (rz >= 6)

    def stage_a(s):
        j, r = s // 2, s % 2

        @pl.when(rz == r)
        def _():
            if j == 0:
                copy_a.wait()
            else:
                rc(shard_at(s, y), shard_at(s, y), s_wa, wa.at[j], p, x).wait_recv()

        @pl.when(rz != r)
        def _():
            z_in(s).wait_recv()

        @pl.when(up_pred(s))
        def _():
            z_up(s).start()

        @pl.when(dn_pred(s))
        def _():
            z_dn(s).start()

        y_up(s).start()
        y_dn(s).start()
        pass_on(s, 0).start()

    def stage_b(s):
        y_up_in(s).wait_recv()
        f_up(s).start()
        pass_on(s, 3).start()
        y_dn_in(s).wait_recv()
        f_dn(s).start()
        pass_on(s, 1).start()

    def stage_c(s):
        f_up_in(s).wait_recv()
        f_dn_in(s).wait_recv()
        pass_on(s, 2).start()

    def product(s, rws):
        j, r = s // 2, s % 2
        prod = lax.dot_general(T[j, rws], W[j, r], (((1,), (1,)), ((), ())),
                               preferred_element_type=F32)
        if j == 0:
            ACC[r, rws] = prod
        else:
            ACC[r, rws] += prod

    def compute(s):
        sib_in(s).wait_recv()
        blk = rows // 2

        def body(i, _):
            product(s, pl.ds(pl.multiple_of(i * blk, blk), blk))
            return 0

        lax.fori_loop(0, 2, body, 0)

    def fin_block(zz, lo, n):
        return FIN.at[lax.rem(zz, 8), lo:lo + n, c]

    def fin_up(h):
        lo, n = (0, 4) if h < 4 else (0, 2)
        ref = fin_block(z + 9 - h, lo, n)
        return rc(ref, ref, s_fnz.at[0, h], fnu.at[h], zu, x)

    def fin_up_in(h):
        lo, n = (0, 4) if h < 4 else (0, 2)
        ref = fin_block(z + 8 - h, lo, n)
        return rc(ref, ref, s_fnz.at[0, h], fnu.at[h], p, x)

    def fin_dn(h):
        lo, n = (0, 4) if h < 4 else (2, 2)
        ref = fin_block(z + h - 1, lo, n)
        return rc(ref, ref, s_fnz.at[1, h], fnd.at[h], zd, x)

    def fin_dn_in(h):
        lo, n = (0, 4) if h < 4 else (2, 2)
        ref = fin_block(z + h, lo, n)
        return rc(ref, ref, s_fnz.at[1, h], fnd.at[h], p, x)

    def fin_sib():
        ref = FIN.at[:, :, c]
        return rc(ref, ref, s_fnc, fnc, sib, x)

    def fin_sib_in():
        ref = FIN.at[:, :, 1 - c]
        return rc(ref, ref, s_fnc, fnc, p, x)

    base_factor = 1.0 / math.sqrt(width_in)
    low_factor = noise_scale / math.sqrt(4 * width_in)
    lanes = lax.broadcasted_iota(jnp.int32, (8, 128), 1)
    sub = lax.broadcasted_iota(jnp.int32, (8, 128), 0)

    def epilogue(m):
        rws = slice(m * mem, (m + 1) * mem)
        codes = ACC[0, rws, half:half + rank16]
        col = lax.broadcasted_iota(jnp.int32, (mem, rank16), 1)
        codes = jnp.where(col // 4 == m, codes, 0.0)
        hi = codes.astype(BF16)
        lo = (codes - hi.astype(F32)).astype(BF16)
        for r in range(2):
            cols = slice(r * half, (r + 1) * half)
            outer = S32[:, pl.ds(pl.multiple_of(x * kw + r * half, 128), half)].astype(BF16)
            low = jnp.dot(hi, outer, preferred_element_type=F32) + jnp.dot(
                lo, outer, preferred_element_type=F32)
            full = ACC[r, rws, 0:half] * base_factor + low * low_factor
            out[rws, cols] = full.astype(BF16)
            part = jnp.sum(full * TG[rws, cols].astype(F32)) / (mem * math.sqrt(width_out))
            FX[0] += jnp.where((sub == e) & (lanes == m), part, 0.0)

    FX[0] = jnp.zeros((8, 128), F32)
    far = (rz >= 3) & (rz <= 6)

    def forward(ms):
        for m in ms:
            (tok_left if m % 2 else tok_right)(m).wait_recv()
            tok_fwd(m).start()

    def fwd_far(*ms):
        @pl.when(far)
        def _():
            forward(ms)

    def fwd_near(*ms):
        @pl.when(jnp.logical_not(far))
        def _():
            forward(ms)

    def fin_hop(h):
        if h == 1:
            for k in range(1, 4):
                fin_y_in(k).wait_recv()
        else:
            fin_up_in(h - 1).wait_recv()
            fin_dn_in(h - 1).wait_recv()
        fin_up(h).start()
        fin_dn(h).start()

    def tokens_in():
        for k in range(1, 4):
            rc(FP, W.at[xslot[k], 0, half:half + rank16], s_fx.at[k], fxs.at[k], p, x).wait_recv()
        for m in (0, 2):
            tok_left(m).wait_recv()

    def fo_hop():
        for k in range(1, 8):
            fo_y_in(k).wait_recv()
        for k in range(1, 8):
            fo_z(k).start()
        FO3[z] = FO2[:, z]

    A, B, C = stage_a, stage_b, stage_c
    A(0)
    A(1)
    B(0)
    A(2)
    A(3)
    fin_hop(1)
    B(1)
    fwd_far(0, 1)
    C(0)
    A(4)
    B(2)
    A(5)
    C(1)
    fwd_far(2, 3)
    fwd_near(0, 1)
    A(6)
    B(3)
    fin_hop(2)
    C(2)
    A(7)
    compute(0)
    B(4)
    C(3)
    compute(1)
    fin_hop(3)
    B(5)
    C(4)
    fwd_near(2, 3)
    B(6)
    fin_hop(4)
    C(5)
    tokens_in()
    compute(2)
    B(7)
    compute(3)
    C(6)
    fo_hop()
    for m in (1, 3):
        tok_right(m).wait_recv()
    compute(4)
    C(7)
    compute(5)
    fin_up_in(4).wait_recv()
    fin_dn_in(4).wait_recv()
    fin_sib().start()
    sib_in(6).wait_recv()
    sib_in(7).wait_recv()
    for pair in ((0, 1), (2, 3)):
        for m in pair:
            tok_fwd(m).wait_recv()
        for m in pair:
            for k in (6, 7):
                product(k, pl.ds(m * mem, mem))
            epilogue(m)

    def g_x(k):
        return rc(FX.at[0], FX.at[k], s_gx.at[k], gx.at[k], p, lax.rem(x + k, 4))

    for k in range(1, 4):
        g_x(k).start()
    for k in range(1, 4):
        g_x(k).wait_recv()
    FY[0] = FX[0] + FX[1] + FX[2] + FX[3]

    def g_y(k):
        return rc(FY.at[0], FY.at[k], s_gy.at[k], gy.at[k], z * 8 + lax.rem(e + k, 8), x)

    for k in range(1, 8):
        g_y(k).start()
    for k in range(1, 8):
        g_y(k).wait_recv()
    plane = FY[0]
    for k in range(1, 8):
        plane = plane + FY[k]
    FP32 = plane
    FZ[z] = FP32

    def g_z(k):
        return rc(FZ.at[z], FZ.at[z], s_gz.at[k], gz.at[k], pop_of(z + k, e), x)

    def g_z_in(k):
        ref = FZ.at[lax.rem(z + 8 - k, 8)]
        return rc(ref, ref, s_gz.at[k], gz.at[k], p, x)

    for k in range(1, 8):
        g_z(k).start()
    for k in range(1, 8):
        fo_z_in(k).wait_recv()
    fin_sib_in().wait_recv()
    for k in range(1, 8):
        g_z_in(k).wait_recv()

    grid = FZ[...].reshape(64, 128)
    mean = jnp.sum(grid) / 256.0
    wide = jnp.broadcast_to(grid[:, None, :], (64, 16, 128)).reshape(1024, 128)
    rr = lax.broadcasted_iota(jnp.int32, (1024, 128), 0)
    cc = lax.broadcasted_iota(jnp.int32, (1024, 128), 1)
    mine = jnp.where(cc == lax.rem(rr, 16) // 4, wide, 0.0)
    centered = jnp.sum(mine, axis=1, keepdims=True) - mean
    scaled = (centered * FO3[...].reshape(1024, 128).astype(F32)).astype(BF16)
    delta = lax.dot_general(scaled, FIN[...].reshape(1024, kw), (((0,), (0,)), ((), ())),
                            preferred_element_type=F32)
    neww[...] = (WL[...].astype(F32) + step_scale / math.sqrt(1024.0) * delta[0:sr]).astype(BF16)

    @pl.when(off != 0)
    def _():
        send_a.wait_send()

    for k in range(1, 4):
        rc(FP, W.at[xslot[k], 0, half:half + rank16], s_fx.at[k], fxs.at[k], p, x).wait_send()
        fin_y(k).wait_send()
        g_x(k).wait_send()
    for m in range(4):
        tok_right(m).wait_send()
        tok_left(m).wait_send()
        tok_fwd(m).wait_send()
    for s in range(NSTEP):
        @pl.when(up_pred(s))
        def _():
            z_up(s).wait_send()

        @pl.when(dn_pred(s))
        def _():
            z_dn(s).wait_send()

        y_up(s).wait_send()
        y_dn(s).wait_send()
        f_up(s).wait_send()
        f_dn(s).wait_send()
        for k in range(4):
            pass_on(s, k).wait_send()
    for h in range(1, 5):
        fin_up(h).wait_send()
        fin_dn(h).wait_send()
    fin_sib().wait_send()
    for k in range(1, 8):
        fo_y(k).wait_send()
        fo_z(k).wait_send()
        g_y(k).wait_send()
        g_z(k).wait_send()


def local(tokens, target, weight, factor_out, factor_in):
    rows, kw = tokens.shape
    sr = weight.shape[0]
    half = 8 * sr
    width = factor_out.shape[2]
    any_spec = pl.BlockSpec(memory_space=pltpu.HBM)
    vm = pl.BlockSpec(memory_space=pltpu.VMEM)
    D = pltpu.SemaphoreType.DMA
    scratch = [
        pltpu.VMEM(factor_out.shape, BF16),
        pltpu.VMEM(factor_in.shape, BF16),
        pltpu.VMEM((4, rows, kw), BF16),
        pltpu.VMEM((4, 2, half + 16, kw), BF16),
        pltpu.VMEM((8, 4, 2, 16, kw), BF16),
        pltpu.VMEM((rows, kw), BF16),
        pltpu.VMEM((sr, kw), BF16),
        pltpu.VMEM((2, rows, half + 16), F32),
        pltpu.VMEM((16, width), F32),
        pltpu.VMEM((8, 8, 16, 128), BF16),
        pltpu.VMEM((8, 8, 16, 128), BF16),
        pltpu.VMEM((8, 8, 16, 128), BF16),
        pltpu.VMEM((16, kw), BF16),
        pltpu.VMEM((4, 8, 128), F32),
        pltpu.VMEM((8, 8, 128), F32),
        pltpu.VMEM((8, 8, 128), F32),
        D((6,)), D((4,)), D((4,)), D((4,)), D((4,)), D((8,)), D((8,)), D((8,)), D((8,)), D((8,)), D((8,)),
        D((4,)), D((4,)), D((5,)), D((5,)), D(()), D((8,)), D((8,)), D((4,)), D((8,)), D((8,)),
        D((2, 4)), D((4,)), D(()), D((6, 8)), D((4, 8)), D((4,)), D((4,)), D((2, 5)), D(()),
        D((8,)), D((8,)), D((4,)), D((8,)), D((8,)),
    ]
    return pl.pallas_call(
        kernel,
        out_shape=(pltpu.VMEM((rows, kw), BF16), pltpu.VMEM((sr, kw), BF16)),
        in_specs=[any_spec] * 5,
        out_specs=(vm, vm),
        scratch_shapes=scratch,
        compiler_params=pltpu.CompilerParams(
            collective_id=0, has_side_effects=True, vmem_limit_bytes=56 * 1024 * 1024),
    )(tokens, target, weight, factor_out, factor_in)


def solution(mesh):
    from jax.sharding import PartitionSpec as P

    in_specs = (
        P("pop", "tp"),
        P("pop", "tp"),
        P("pop", "tp"),
        P("pop", None, None),
        P("pop", None, "tp"),
    )
    out_specs = (P("pop", "tp"), P("pop", "tp"))
    return jax.shard_map(local, mesh=mesh, in_specs=in_specs, out_specs=out_specs, check_vma=False)
```

```python
import math

import jax
import jax.numpy as jnp
from jax import lax
from jax.experimental import pallas as pl
from jax.experimental.pallas import tpu as pltpu

noise_scale = 0.25
step_scale = 10.0

F32 = jnp.float32
BF16 = jnp.bfloat16
NX, NY, NZ = 4, 4, 8
NSTEP = 8


def kernel(tok, tgt, wt, fo_hbm, fin_hbm, out, neww,
           fo, fin, T, W, FIN, TG, WL, ACC, S32, FOS, FO2, FO3, FP, FX, FZ,
           loc, tr, tl, tf, wa, wz, yin, ff, d2, fxs, fny, fnu, fnd, fnc,
           foy, foz, gx, gz,
           s_tok, s_tf, s_wa, s_z, s_y, s_f, s_d2, s_fx, s_fny, s_fnz, s_fnc, s_foy, s_foz, s_gx, s_gz):
    p = lax.axis_index("pop")
    x = lax.axis_index("tp")
    z = p // 8
    e = p % 8
    y = e // 2
    c = e % 2
    rows, kw = tok.shape
    mem = rows // 4
    sr = wt.shape[0]
    half = 8 * sr
    rank16 = 16
    width_in = kw * NX
    width_out = width_in

    def pop_of(zz, ee):
        return lax.rem(zz, 8) * 8 + lax.rem(ee, 8)

    def rc(src, dst, ss, rs, pop, tp):
        return pltpu.make_async_remote_copy(
            src_ref=src, dst_ref=dst, send_sem=ss, recv_sem=rs,
            device_id={"pop": pop, "tp": tp}, device_id_type=pl.DeviceIdType.MESH)

    xr = lax.rem(x + 1, 4)
    xl = lax.rem(x + 3, 4)
    zu = pop_of(z + 1, e)
    zd = pop_of(z + 7, e)
    yup = z * 8 + lax.rem(y + 1, 4) * 2 + c
    ydn = z * 8 + lax.rem(y + 3, 4) * 2 + c
    sib = z * 8 + y * 2 + (1 - c)

    l_wl = pltpu.make_async_copy(wt, WL, loc.at[0])
    l_t0 = pltpu.make_async_copy(tok, T.at[0], loc.at[1])
    l_tg = pltpu.make_async_copy(tgt, TG, loc.at[2])
    l_fi = pltpu.make_async_copy(fin_hbm, fin, loc.at[4])
    l_fo = pltpu.make_async_copy(fo_hbm, fo, loc.at[5])
    l_fi.start()
    l_fo.start()
    l_wl.start()
    l_t0.start()
    l_tg.start()

    bar = pltpu.get_barrier_semaphore()
    def xy_peer(k):
        return z * 8 + lax.rem(y + k // 4, 4) * 2 + c, lax.rem(x + k % 4, 4)

    def zc_peer(k):
        return lax.rem(z + k % 8, 8) * 8 + y * 2 + lax.rem(c + k // 8, 2)

    partners = [xy_peer(k) for k in range(1, 16)] + [(zc_peer(k), x) for k in range(1, 16)]
    partners += [(z * 8 + lax.rem(y + k, 4) * 2 + 1 - c, x) for k in range(1, 4)]
    for pop, tp in partners:
        pl.semaphore_signal(bar, inc=1, device_id={"pop": pop, "tp": tp},
                            device_id_type=pl.DeviceIdType.MESH)
    l_fi.wait()
    for i in range(4):
        S32[4 * i:4 * i + 4, 0:kw] = fin[i].astype(F32)
    fin16 = S32[:, 0:kw].astype(BF16)
    FP[...] = fin16
    FIN[z, y, c] = fin16
    W[0, 0, half:half + rank16] = fin16
    pl.semaphore_wait(bar, 33)

    zt = z // 2
    r_own = lax.rem(z, 2)
    off = lax.rem(x - zt + 4, 4)
    slot = off + off // 2 - 2 * (off // 3)
    shard = pl.ds(pl.multiple_of(e * sr, 16), sr)
    send_a = rc(wt, W.at[slot, r_own, shard], s_wa, wa.at[slot], p, zt)
    copy_a = pltpu.make_async_copy(wt, W.at[0, r_own, shard], loc.at[3])

    @pl.when(off == 0)
    def _():
        copy_a.start()

    @pl.when(off != 0)
    def _():
        send_a.start()

    xslot = {1: 2, 2: 3, 3: 1}
    for k in range(1, 4):
        rc(FP, W.at[xslot[k], 0, half:half + rank16], s_fx, fxs.at[k], p, lax.rem(x + k, 4)).start()

    def chunk(m):
        return pl.ds(m * mem, mem)

    def tok_right(m):
        return rc(tok.at[chunk(m)], T.at[2, chunk(m)], s_tok.at[0, m], tr.at[m], p, xr)

    def tok_left(m):
        return rc(tok.at[chunk(m)], T.at[1, chunk(m)], s_tok.at[1, m], tl.at[m], p, xl)

    small = mem // 2
    pieces = ((0, 0, mem), (3, 3 * mem, mem), (1, mem, small), (2, 2 * mem + small, small),
              (1, mem + small, small), (2, 2 * mem, small))

    def tok_fwd(i):
        m, first, n = pieces[i]
        rws = pl.ds(first, n)
        side, to = (1, xl) if m >= 2 else (2, xr)
        return rc(T.at[side, rws], T.at[3, rws], s_tf.at[i], tf.at[i], p, to)

    for m in range(4):
        tok_right(m).start()
        tok_left(3 - m).start()

    def fin_y(k):
        return rc(FP, FIN.at[z, y, c], s_fny, fny.at[k],
                  z * 8 + lax.rem(y + k, 4) * 2 + c, x)

    def fin_y_in(k):
        return rc(FP, FIN.at[z, lax.rem(y + 4 - k, 4), c], s_fny, fny.at[k], p, x)

    for k in range(1, 4):
        fin_y(k).start()

    def fo_y(k):
        ee = lax.rem(e + k, 8)
        return rc(FOS.at[ee], FO2.at[e], s_foy, foy.at[k], z * 8 + ee, x)

    def fo_y_in(k):
        return rc(FOS.at[0], FO2.at[lax.rem(e + 8 - k, 8)], s_foy, foy.at[k], p, x)

    def fo_cut():
        l_fo.wait()
        for i in range(4):
            S32[4 * i:4 * i + 4, :] = fo[i].astype(F32)
        grp = 8 * sr
        sel_row = lax.broadcasted_iota(jnp.int32, (grp, 1024), 0)
        sel_col = lax.broadcasted_iota(jnp.int32, (grp, 1024), 1)
        lane = lax.rem(sel_col, 128)
        want = (sel_col // 128) * sr + lane
        sel = jnp.where((sel_row == want) & (lane < sr), 1.0, 0.0).astype(BF16)
        for g in range(8):
            cut = jnp.dot(S32[:, g * grp:(g + 1) * grp].astype(BF16), sel,
                          preferred_element_type=F32).astype(BF16)
            for d in range(8):
                FOS[d, g] = cut[:, d * 128:(d + 1) * 128]
        FO2[e] = FOS[e]
        for k in range(1, 8):
            fo_y(k).start()

    def fo_z(k):
        zz = lax.rem(z + k, 8)
        return rc(FO2.at[:, zz], FO3.at[z], s_foz, foz.at[k], zz * 8 + e, x)

    def fo_z_in(k):
        return rc(FO2.at[:, 0], FO3.at[lax.rem(z + 8 - k, 8)], s_foz, foz.at[k], p, x)

    l_wl.wait()
    l_t0.wait()
    l_tg.wait()

    rz = lax.rem(z + 8 - 2 * x, 8)

    def shard_at(s, yy, h=None):
        q = lax.rem(yy, 4) * 2 + c
        rws = pl.ds(pl.multiple_of(q * sr, 16), sr)
        if h is None:
            return W.at[s // 2, s % 2, rws]
        return W.at[s // 2, s % 2, rws, pl.ds(h * (kw // 2), kw // 2)]

    def piece(s, yy, h, ss, rs, pop):
        return rc(shard_at(s, yy, h), shard_at(s, yy, h), ss, rs, pop, x)

    def z_send(s, h, d):
        return piece(s, y, h, s_z.at[d, 2 * s + h], wz.at[2 * s + h], (zu, zd)[d])

    def z_in(s, h):
        return piece(s, y, h, s_z.at[0, 2 * s + h], wz.at[2 * s + h], p)

    def y_send(s, h, d):
        return piece(s, y, h, s_y.at[d], yin.at[d, 2 * s + h], (yup, ydn)[d])

    def y_in(s, h, d):
        return piece(s, y + (3, 1)[d], h, s_y.at[d], yin.at[d, 2 * s + h], p)

    def f_send(s, d):
        return piece(s, y + (3, 1)[d], d, s_f.at[d], ff.at[d, s], (yup, ydn)[d])

    def f_in(s, d):
        return piece(s, y + 2, d, s_f.at[d], ff.at[d, s], p)

    def pass_on(s, k):
        return rc(shard_at(s, y + k), shard_at(s, y + k), s_d2.at[s], d2.at[s], sib, x)

    def sib_in(s):
        whole = W.at[s // 2, s % 2, 0:4 * sr]
        return rc(whole, whole, s_d2.at[s], d2.at[s], p, x)

    def z_pred(s, d):
        if d == 0:
            return rz <= 3 if s % 2 == 0 else (rz >= 1) & (rz <= 3)
        return (rz == 0) | (rz >= 6) if s % 2 == 0 else (rz <= 1) | (rz >= 6)

    def stage_a(s, h):
        j, r = s // 2, s % 2

        if h == 0:
            @pl.when(rz == r)
            def _():
                if j == 0:
                    copy_a.wait()
                else:
                    rc(shard_at(s, y), shard_at(s, y), s_wa, wa.at[j], p, x).wait_recv()

        @pl.when(rz != r)
        def _():
            z_in(s, h).wait_recv()

        for d in range(2):
            @pl.when(z_pred(s, d))
            def _():
                z_send(s, h, d).start()

        for d in range(2):
            y_send(s, h, d).start()
        if h == 1:
            pass_on(s, 0).start()

    def stage_b(s, h):
        for d in range(2):
            y_in(s, h, d).wait_recv()
            if d == h:
                f_send(s, d).start()
        if h == 1:
            pass_on(s, 3).start()
            pass_on(s, 1).start()

    def stage_c(s):
        for d in range(2):
            f_in(s, d).wait_recv()
        pass_on(s, 2).start()

    def product(s, rws):
        j, r = s // 2, s % 2
        prod = lax.dot_general(T[j, rws], W[j, r], (((1,), (1,)), ((), ())),
                               preferred_element_type=F32)
        if j == 0:
            ACC[r, rws] = prod
        else:
            ACC[r, rws] += prod

    def compute(s):
        sib_in(s).wait_recv()
        blk = rows // 2

        def body(i, _):
            product(s, pl.ds(pl.multiple_of(i * blk, blk), blk))
            return 0

        lax.fori_loop(0, 2, body, 0)

    def fin_block(zz, lo, n):
        return FIN.at[lax.rem(zz, 8), lo:lo + n, c]

    def fin_up(h):
        lo, n = (0, 4) if h < 4 else (0, 2)
        ref = fin_block(z + 9 - h, lo, n)
        return rc(ref, ref, s_fnz.at[0, h], fnu.at[h], zu, x)

    def fin_up_in(h):
        lo, n = (0, 4) if h < 4 else (0, 2)
        ref = fin_block(z + 8 - h, lo, n)
        return rc(ref, ref, s_fnz.at[0, h], fnu.at[h], p, x)

    def fin_dn(h):
        lo, n = (0, 4) if h < 4 else (2, 2)
        ref = fin_block(z + h - 1, lo, n)
        return rc(ref, ref, s_fnz.at[1, h], fnd.at[h], zd, x)

    def fin_dn_in(h):
        lo, n = (0, 4) if h < 4 else (2, 2)
        ref = fin_block(z + h, lo, n)
        return rc(ref, ref, s_fnz.at[1, h], fnd.at[h], p, x)

    def fin_sib():
        ref = FIN.at[:, :, c]
        return rc(ref, ref, s_fnc, fnc, sib, x)

    def fin_sib_in():
        ref = FIN.at[:, :, 1 - c]
        return rc(ref, ref, s_fnc, fnc, p, x)

    base_factor = 1.0 / math.sqrt(width_in)
    low_factor = noise_scale / math.sqrt(4 * width_in)
    lanes = lax.broadcasted_iota(jnp.int32, (8, 128), 1)
    sub = lax.broadcasted_iota(jnp.int32, (8, 128), 0)

    def epilogue(m, first, n):
        rws = slice(first, first + n)
        codes = ACC[0, rws, half:half + rank16]
        col = lax.broadcasted_iota(jnp.int32, (n, rank16), 1)
        codes = jnp.where(col // 4 == m, codes, 0.0)
        hi = codes.astype(BF16)
        lo = (codes - hi.astype(F32)).astype(BF16)
        for r in range(2):
            cols = slice(r * half, (r + 1) * half)
            outer = S32[:, pl.ds(pl.multiple_of(x * kw + r * half, 128), half)].astype(BF16)
            low = jnp.dot(hi, outer, preferred_element_type=F32) + jnp.dot(
                lo, outer, preferred_element_type=F32)
            full = ACC[r, rws, 0:half] * base_factor + low * low_factor
            out[rws, cols] = full.astype(BF16)
            part = jnp.sum(full * TG[rws, cols].astype(F32)) / (mem * math.sqrt(width_out))
            FX[0] += jnp.where((sub == e) & (lanes == m), part, 0.0)

    FX[0] = jnp.zeros((8, 128), F32)

    zone = (rz <= 1, (rz == 2) | (rz == 7), (rz >= 3) & (rz <= 6))

    def fwd(which, pair):
        @pl.when(zone[which])
        def _():
            for m in ((0, 3), (1, 2))[pair]:
                (tok_left if m >= 2 else tok_right)(m).wait_recv()
            for i in ((0, 1), (2, 3, 4, 5))[pair]:
                tok_fwd(i).start()

    def fin_hop(h):
        if h == 1:
            for k in range(1, 4):
                fin_y_in(k).wait_recv()
        else:
            fin_up_in(h - 1).wait_recv()
            fin_dn_in(h - 1).wait_recv()
        fin_up(h).start()
        fin_dn(h).start()

    def tokens_in():
        for k in range(1, 4):
            rc(FP, W.at[xslot[k], 0, half:half + rank16], s_fx, fxs.at[k], p, x).wait_recv()
        for m in (0, 1):
            tok_left(m).wait_recv()

    def fo_hop():
        for k in range(1, 8):
            fo_y_in(k).wait_recv()
        for k in range(1, 8):
            fo_z(k).start()
        FO3[z] = FO2[:, z]

    A, B, C = stage_a, stage_b, stage_c
    A(0, 0)
    A(0, 1)
    fo_cut()
    A(1, 0)
    B(0, 0)
    A(1, 1)
    B(0, 1)
    fwd(2, 0)
    A(2, 0)
    fin_hop(1)
    B(1, 0)
    A(2, 1)
    C(0)
    B(1, 1)
    A(3, 0)
    fwd(1, 0)
    A(3, 1)
    B(2, 0)
    C(1)
    A(4, 0)
    B(2, 1)
    fwd(2, 1)
    A(4, 1)
    B(3, 0)
    fwd(0, 0)
    A(5, 0)
    C(2)
    fin_hop(2)
    B(3, 1)
    A(5, 1)
    A(6, 0)
    B(4, 0)
    C(3)
    fwd(1, 1)
    A(6, 1)
    compute(0)
    B(4, 1)
    A(7, 0)
    compute(1)
    B(5, 0)
    A(7, 1)
    C(4)
    fwd(0, 1)
    B(5, 1)
    fin_hop(3)
    B(6, 0)
    C(5)
    B(6, 1)
    tokens_in()
    compute(2)
    B(7, 0)
    C(6)
    compute(3)
    B(7, 1)
    for m in (2, 3):
        tok_right(m).wait_recv()
    compute(4)
    compute(5)
    fin_hop(4)
    C(7)
    fo_hop()
    sib_in(6).wait_recv()
    sib_in(7).wait_recv()
    for pair in ((0, 1), (2, 3), (4, 5)):
        for i in pair:
            tok_fwd(i).wait_recv()
        if pair[0] == 4:
            for k in (6, 7):
                product(k, pl.ds(mem + small, mem))
        for i in pair:
            m, first, n = pieces[i]
            if pair[0] < 4:
                for k in (6, 7):
                    product(k, pl.ds(first, n))
            epilogue(m, first, n)
        if pair[0] == 0:
            fin_up_in(4).wait_recv()
            fin_dn_in(4).wait_recv()
            fin_sib().start()

    def g_x(k):
        pop, tp = xy_peer(k)
        return rc(FX.at[0], FX.at[k], s_gx, gx.at[k], pop, tp)

    for k in range(1, 16):
        g_x(k).start()
    for k in range(1, 16):
        g_x(k).wait_recv()
    plane = FX[0]
    for k in range(1, 16):
        plane = plane + FX[k]
    FZ[z * 2 + c] = plane

    def g_z(k):
        ref = FZ.at[z * 2 + c]
        return rc(ref, ref, s_gz, gz.at[k], zc_peer(k), x)

    def g_z_in(k):
        ref = FZ.at[lax.rem(z + 8 - k % 8, 8) * 2 + lax.rem(c + k // 8, 2)]
        return rc(ref, ref, s_gz, gz.at[k], p, x)

    for k in range(1, 16):
        g_z(k).start()
    def left(ref, sem):
        rc(ref, ref, sem, fnc, p, x).wait_send()

    @pl.when(off != 0)
    def _():
        send_a.wait_send()

    left(FIN.at[0, 0:3, 0], s_fx)
    left(FIN.at[0, 0:3, 0], s_fny)
    for m in range(4):
        tok_right(m).wait_send()
        tok_left(m).wait_send()
    for i in range(6):
        tok_fwd(i).wait_send()
    for s in range(NSTEP):
        for d in range(2):
            for h in range(2):
                @pl.when(z_pred(s, d))
                def _():
                    z_send(s, h, d).wait_send()
        left(W.at[0, 0, 0:4 * sr], s_d2.at[s])
    for d in range(2):
        left(W.at[0, 0, 0:8 * sr], s_y.at[d])
        left(W.at[0, 0, 0:4 * sr], s_f.at[d])
    for h in range(1, 5):
        fin_up(h).wait_send()
        fin_dn(h).wait_send()
    fin_sib().wait_send()
    left(FOS.at[0:7], s_foy)
    left(FO3.at[0:7], s_foz)
    for k in range(1, 8):
        fo_z_in(k).wait_recv()
    fin_sib_in().wait_recv()
    left(FX.at[0:15], s_gx)
    left(FZ.at[0:15], s_gz)
    for k in range(1, 16):
        g_z_in(k).wait_recv()

    tiles = FZ[...].reshape(8, 2, 8, 128)
    grid = (tiles[:, 0] + tiles[:, 1]).reshape(64, 128)
    mean = jnp.sum(grid) / 256.0
    wide = jnp.broadcast_to(grid[:, None, :], (64, 16, 128)).reshape(1024, 128)
    rr = lax.broadcasted_iota(jnp.int32, (1024, 128), 0)
    cc = lax.broadcasted_iota(jnp.int32, (1024, 128), 1)
    mine = jnp.where(cc == lax.rem(rr, 16) // 4, wide, 0.0)
    centered = jnp.sum(mine, axis=1, keepdims=True) - mean
    scaled = (centered * FO3[...].reshape(1024, 128).astype(F32)).astype(BF16)
    delta = lax.dot_general(scaled, FIN[...].reshape(1024, kw), (((0,), (0,)), ((), ())),
                            preferred_element_type=F32)
    neww[...] = (WL[...].astype(F32) + step_scale / math.sqrt(1024.0) * delta[0:sr]).astype(BF16)


def local(tokens, target, weight, factor_out, factor_in):
    rows, kw = tokens.shape
    sr = weight.shape[0]
    half = 8 * sr
    width = factor_out.shape[2]
    any_spec = pl.BlockSpec(memory_space=pltpu.HBM)
    vm = pl.BlockSpec(memory_space=pltpu.VMEM)
    D = pltpu.SemaphoreType.DMA
    scratch = [
        pltpu.VMEM(factor_out.shape, BF16),
        pltpu.VMEM(factor_in.shape, BF16),
        pltpu.VMEM((4, rows, kw), BF16),
        pltpu.VMEM((4, 2, half + 16, kw), BF16),
        pltpu.VMEM((8, 4, 2, 16, kw), BF16),
        pltpu.VMEM((rows, kw), BF16),
        pltpu.VMEM((sr, kw), BF16),
        pltpu.VMEM((2, rows, half + 16), F32),
        pltpu.VMEM((16, width), F32),
        pltpu.VMEM((8, 8, 16, 128), BF16),
        pltpu.VMEM((8, 8, 16, 128), BF16),
        pltpu.VMEM((8, 8, 16, 128), BF16),
        pltpu.VMEM((16, kw), BF16),
        pltpu.VMEM((16, 8, 128), F32),
        pltpu.VMEM((16, 8, 128), F32),
        D((6,)), D((4,)), D((4,)), D((6,)), D((4,)), D((16,)), D((2, 16)), D((2, 8)), D((8,)),
        D((4,)), D((4,)), D((5,)), D((5,)), D(()), D((8,)), D((8,)), D((16,)), D((16,)),
        D((2, 4)), D((6,)), D(()), D((2, 16)), D((2,)), D((2,)), D((8,)), D(()), D(()), D((2, 5)), D(()),
        D(()), D(()), D(()), D(()),
    ]
    return pl.pallas_call(
        kernel,
        out_shape=(pltpu.VMEM((rows, kw), BF16), pltpu.VMEM((sr, kw), BF16)),
        in_specs=[any_spec] * 5,
        out_specs=(vm, vm),
        scratch_shapes=scratch,
        compiler_params=pltpu.CompilerParams(
            collective_id=0, has_side_effects=True, vmem_limit_bytes=56 * 1024 * 1024),
    )(tokens, target, weight, factor_out, factor_in)


def solution(mesh):
    from jax.sharding import PartitionSpec as P

    in_specs = (
        P("pop", "tp"),
        P("pop", "tp"),
        P("pop", "tp"),
        P("pop", None, None),
        P("pop", None, "tp"),
    )
    out_specs = (P("pop", "tp"), P("pop", "tp"))
    return jax.shard_map(local, mesh=mesh, in_specs=in_specs, out_specs=out_specs, check_vma=False)
```

```python
import math

import jax
import jax.numpy as jnp
from jax import lax
from jax.experimental import pallas as pl
from jax.experimental.pallas import tpu as pltpu

noise_scale = 0.25
step_scale = 10.0

F32 = jnp.float32
BF16 = jnp.bfloat16
NX, NY, NZ = 4, 4, 8
NSTEP = 8


def kernel(tok, tgt, wt, fo_hbm, fin_hbm, out, neww,
           fo, fin, T, W, FIN, TG, WL, ACC, S32, FOS, FO2, FO3, FP, FX, FZ,
           loc, tr, tl, tf, wa, wz, yin, ff, d2, fxs, fny, fnu, fnd, fnc,
           foy, foz, gx, gz,
           s_tok, s_tf, s_wa, s_z, s_y, s_f, s_d2, s_fx, s_fny, s_fnz, s_fnc, s_foy, s_foz, s_gx, s_gz):
    p = lax.axis_index("pop")
    x = lax.axis_index("tp")
    z = p // 8
    e = p % 8
    y = e // 2
    c = e % 2
    rows, kw = tok.shape
    mem = rows // 4
    sr = wt.shape[0]
    half = 8 * sr
    rank16 = 16
    width_in = kw * NX
    width_out = width_in

    def pop_of(zz, ee):
        return lax.rem(zz, 8) * 8 + lax.rem(ee, 8)

    def rc(src, dst, ss, rs, pop, tp):
        return pltpu.make_async_remote_copy(
            src_ref=src, dst_ref=dst, send_sem=ss, recv_sem=rs,
            device_id={"pop": pop, "tp": tp}, device_id_type=pl.DeviceIdType.MESH)

    xr = lax.rem(x + 1, 4)
    xl = lax.rem(x + 3, 4)
    zu = pop_of(z + 1, e)
    zd = pop_of(z + 7, e)
    yup = z * 8 + lax.rem(y + 1, 4) * 2 + c
    ydn = z * 8 + lax.rem(y + 3, 4) * 2 + c
    sib = z * 8 + y * 2 + (1 - c)

    l_wl = pltpu.make_async_copy(wt, WL, loc.at[0])
    l_t0 = pltpu.make_async_copy(tok, T.at[0], loc.at[1])
    l_tg = pltpu.make_async_copy(tgt, TG, loc.at[2])
    l_fi = pltpu.make_async_copy(fin_hbm, fin, loc.at[4])
    l_fo = pltpu.make_async_copy(fo_hbm, fo, loc.at[5])
    l_fi.start()
    l_fo.start()
    l_wl.start()
    l_t0.start()
    l_tg.start()

    bar = pltpu.get_barrier_semaphore()
    def xy_peer(k):
        return z * 8 + lax.rem(y + k // 4, 4) * 2 + c, lax.rem(x + k % 4, 4)

    def zc_peer(k):
        return lax.rem(z + k % 8, 8) * 8 + y * 2 + lax.rem(c + k // 8, 2)

    partners = [xy_peer(k) for k in range(1, 16)] + [(zc_peer(k), x) for k in range(1, 16)]
    partners += [(z * 8 + lax.rem(y + k, 4) * 2 + 1 - c, x) for k in range(1, 4)]
    for pop, tp in partners:
        pl.semaphore_signal(bar, inc=1, device_id={"pop": pop, "tp": tp},
                            device_id_type=pl.DeviceIdType.MESH)
    l_fi.wait()
    for i in range(4):
        S32[4 * i:4 * i + 4, 0:kw] = fin[i].astype(F32)
    fin16 = S32[:, 0:kw].astype(BF16)
    FP[...] = fin16
    FIN[z, y, c] = fin16
    W[0, 0, half:half + rank16] = fin16
    pl.semaphore_wait(bar, 33)

    zt = z // 2
    r_own = lax.rem(z, 2)
    off = lax.rem(x - zt + 4, 4)
    slot = off + off // 2 - 2 * (off // 3)
    shard = pl.ds(pl.multiple_of(e * sr, 16), sr)
    send_a = rc(wt, W.at[slot, r_own, shard], s_wa, wa.at[slot], p, zt)
    copy_a = pltpu.make_async_copy(wt, W.at[0, r_own, shard], loc.at[3])

    @pl.when(off == 0)
    def _():
        copy_a.start()

    @pl.when(off != 0)
    def _():
        send_a.start()

    xslot = {1: 2, 2: 3, 3: 1}
    for k in range(1, 4):
        rc(FP, W.at[xslot[k], 0, half:half + rank16], s_fx, fxs, p, lax.rem(x + k, 4)).start()

    def chunk(m):
        return pl.ds(m * mem, mem)

    def tok_right(m):
        return rc(tok.at[chunk(m)], T.at[2, chunk(m)], s_tok, tr.at[m], p, xr)

    def tok_left(m):
        return rc(tok.at[chunk(m)], T.at[1, chunk(m)], s_tok, tl.at[m], p, xl)

    small = mem // 2
    pieces = ((0, 0, mem), (3, 3 * mem, mem), (1, mem, small), (2, 2 * mem + small, small),
              (1, mem + small, small), (2, 2 * mem, small))

    def tok_fwd(i):
        m, first, n = pieces[i]
        rws = pl.ds(first, n)
        side, to = (1, xl) if m >= 2 else (2, xr)
        return rc(T.at[side, rws], T.at[3, rws], s_tf, tf.at[i], p, to)

    for m in range(4):
        tok_right(m).start()
        tok_left(3 - m).start()

    def fin_y(k):
        return rc(FP, FIN.at[z, y, c], s_fny, fny,
                  z * 8 + lax.rem(y + k, 4) * 2 + c, x)

    for k in range(1, 4):
        fin_y(k).start()

    def fo_y(k):
        ee = lax.rem(e + k, 8)
        return rc(FOS.at[ee], FO2.at[e], s_foy, foy, z * 8 + ee, x)

    def fo_cut():
        l_fo.wait()
        for i in range(4):
            S32[4 * i:4 * i + 4, :] = fo[i].astype(F32)
        grp = 8 * sr
        sel_row = lax.broadcasted_iota(jnp.int32, (grp, 1024), 0)
        sel_col = lax.broadcasted_iota(jnp.int32, (grp, 1024), 1)
        lane = lax.rem(sel_col, 128)
        want = (sel_col // 128) * sr + lane
        sel = jnp.where((sel_row == want) & (lane < sr), 1.0, 0.0).astype(BF16)
        for g in range(8):
            cut = jnp.dot(S32[:, g * grp:(g + 1) * grp].astype(BF16), sel,
                          preferred_element_type=F32).astype(BF16)
            for d in range(8):
                FOS[d, g] = cut[:, d * 128:(d + 1) * 128]
        FO2[e] = FOS[e]
        for k in range(1, 8):
            fo_y(k).start()

    def fo_z(k):
        zz = lax.rem(z + k, 8)
        return rc(FO2.at[:, zz], FO3.at[z], s_foz, foz, zz * 8 + e, x)

    l_wl.wait()
    l_t0.wait()
    l_tg.wait()

    rz = lax.rem(z + 8 - 2 * x, 8)

    def shard_at(s, yy, h=None):
        q = lax.rem(yy, 4) * 2 + c
        rws = pl.ds(pl.multiple_of(q * sr, 16), sr)
        if h is None:
            return W.at[s // 2, s % 2, rws]
        return W.at[s // 2, s % 2, rws, pl.ds(h * (kw // 2), kw // 2)]

    def piece(s, yy, h, ss, rs, pop):
        return rc(shard_at(s, yy, h), shard_at(s, yy, h), ss, rs, pop, x)

    def z_send(s, h, d):
        return piece(s, y, h, s_z.at[d], wz.at[2 * s + h], (zu, zd)[d])

    def z_in(s, h):
        return piece(s, y, h, s_z.at[0], wz.at[2 * s + h], p)

    def y_send(s, h, d):
        return piece(s, y, h, s_y.at[d], yin.at[2 * s + h], (yup, ydn)[d])

    def f_send(s, d):
        return piece(s, y + (3, 1)[d], d, s_f.at[d], ff.at[s], (yup, ydn)[d])

    def arrived(ref, sem):
        rc(ref, ref, s_wa, sem, p, x).wait_recv()

    def pass_on(s, k):
        return rc(shard_at(s, y + k), shard_at(s, y + k), s_d2, d2.at[s], sib, x)

    def sib_in(s):
        whole = W.at[s // 2, s % 2, 0:4 * sr]
        return rc(whole, whole, s_d2, d2.at[s], p, x)

    def z_pred(s, d):
        if d == 0:
            return rz <= 3 if s % 2 == 0 else (rz >= 1) & (rz <= 3)
        return (rz == 0) | (rz >= 6) if s % 2 == 0 else (rz <= 1) | (rz >= 6)

    def stage_a(s, h):
        j, r = s // 2, s % 2

        if h == 0:
            @pl.when(rz == r)
            def _():
                if j == 0:
                    copy_a.wait()
                else:
                    rc(shard_at(s, y), shard_at(s, y), s_wa, wa.at[j], p, x).wait_recv()

        @pl.when(rz != r)
        def _():
            z_in(s, h).wait_recv()

        for d in range(2):
            @pl.when(z_pred(s, d))
            def _():
                z_send(s, h, d).start()

        for d in range(2):
            y_send(s, h, d).start()
        if h == 1:
            pass_on(s, 0).start()

    def stage_b(s, h):
        arrived(W.at[0, 0, 0:2 * sr, 0:kw // 2], yin.at[2 * s + h])
        f_send(s, h).start()
        if h == 1:
            pass_on(s, 3).start()
            pass_on(s, 1).start()

    def stage_c(s):
        arrived(shard_at(s, y + 2), ff.at[s])
        pass_on(s, 2).start()

    def product(s, rws):
        j, r = s // 2, s % 2
        prod = lax.dot_general(T[j, rws], W[j, r], (((1,), (1,)), ((), ())),
                               preferred_element_type=F32)
        if j == 0:
            ACC[r, rws] = prod
        else:
            ACC[r, rws] += prod

    def compute(s):
        sib_in(s).wait_recv()
        blk = rows // 2

        def body(i, _):
            product(s, pl.ds(pl.multiple_of(i * blk, blk), blk))
            return 0

        lax.fori_loop(0, 2, body, 0)

    def fin_block(zz, lo, n):
        return FIN.at[lax.rem(zz, 8), lo:lo + n, c]

    def fin_up(h):
        lo, n = (0, 4) if h < 4 else (0, 2)
        ref = fin_block(z + 9 - h, lo, n)
        return rc(ref, ref, s_fnz, fnu.at[h], zu, x)

    def fin_up_in(h):
        lo, n = (0, 4) if h < 4 else (0, 2)
        ref = fin_block(z + 8 - h, lo, n)
        return rc(ref, ref, s_fnz, fnu.at[h], p, x)

    def fin_dn(h):
        lo, n = (0, 4) if h < 4 else (2, 2)
        ref = fin_block(z + h - 1, lo, n)
        return rc(ref, ref, s_fnz, fnd.at[h], zd, x)

    def fin_dn_in(h):
        lo, n = (0, 4) if h < 4 else (2, 2)
        ref = fin_block(z + h, lo, n)
        return rc(ref, ref, s_fnz, fnd.at[h], p, x)

    def fin_sib():
        ref = FIN.at[:, :, c]
        return rc(ref, ref, s_fnc, fnc, sib, x)

    def fin_sib_in():
        ref = FIN.at[:, :, 1 - c]
        return rc(ref, ref, s_fnc, fnc, p, x)

    base_factor = 1.0 / math.sqrt(width_in)
    low_factor = noise_scale / math.sqrt(4 * width_in)
    lanes = lax.broadcasted_iota(jnp.int32, (8, 128), 1)
    sub = lax.broadcasted_iota(jnp.int32, (8, 128), 0)

    def epilogue(m, first, n):
        rws = slice(first, first + n)
        codes = ACC[0, rws, half:half + rank16]
        col = lax.broadcasted_iota(jnp.int32, (n, rank16), 1)
        codes = jnp.where(col // 4 == m, codes, 0.0)
        hi = codes.astype(BF16)
        lo = (codes - hi.astype(F32)).astype(BF16)
        for r in range(2):
            cols = slice(r * half, (r + 1) * half)
            outer = S32[:, pl.ds(pl.multiple_of(x * kw + r * half, 128), half)].astype(BF16)
            low = jnp.dot(hi, outer, preferred_element_type=F32) + jnp.dot(
                lo, outer, preferred_element_type=F32)
            full = ACC[r, rws, 0:half] * base_factor + low * low_factor
            out[rws, cols] = full.astype(BF16)
            part = jnp.sum(full * TG[rws, cols].astype(F32)) / (mem * math.sqrt(width_out))
            FX[0] += jnp.where((sub == e) & (lanes == m), part, 0.0)

    FX[0] = jnp.zeros((8, 128), F32)

    zone = (rz <= 1, (rz == 2) | (rz == 7), (rz >= 3) & (rz <= 6))

    def fwd(which, pair):
        @pl.when(zone[which])
        def _():
            for m in ((0, 3), (1, 2))[pair]:
                (tok_left if m >= 2 else tok_right)(m).wait_recv()
            for i in ((0, 1), (2, 3, 4, 5))[pair]:
                tok_fwd(i).start()

    def fin_hop(h):
        if h == 1:
            arrived(FIN.at[z, 0:3, c], fny)
        else:
            fin_up_in(h - 1).wait_recv()
            fin_dn_in(h - 1).wait_recv()
        fin_up(h).start()
        fin_dn(h).start()

    def tokens_in():
        arrived(W.at[0, 0, 0:3 * rank16], fxs)
        for m in (0, 1):
            tok_left(m).wait_recv()

    def fo_hop():
        arrived(FO2.at[0:7], foy)
        for k in range(1, 8):
            fo_z(k).start()
        FO3[z] = FO2[:, z]

    A, B, C = stage_a, stage_b, stage_c
    A(0, 0)
    A(0, 1)
    fo_cut()
    A(1, 0)
    B(0, 0)
    A(1, 1)
    B(0, 1)
    fwd(2, 0)
    A(2, 0)
    fin_hop(1)
    B(1, 0)
    A(2, 1)
    C(0)
    B(1, 1)
    A(3, 0)
    fwd(1, 0)
    A(3, 1)
    B(2, 0)
    C(1)
    A(4, 0)
    B(2, 1)
    fwd(2, 1)
    A(4, 1)
    B(3, 0)
    fwd(0, 0)
    A(5, 0)
    C(2)
    fin_hop(2)
    B(3, 1)
    A(5, 1)
    A(6, 0)
    B(4, 0)
    C(3)
    fwd(1, 1)
    A(6, 1)
    compute(0)
    B(4, 1)
    A(7, 0)
    compute(1)
    B(5, 0)
    A(7, 1)
    C(4)
    fwd(0, 1)
    B(5, 1)
    fin_hop(3)
    B(6, 0)
    C(5)
    B(6, 1)
    tokens_in()
    compute(2)
    B(7, 0)
    C(6)
    compute(3)
    B(7, 1)
    for m in (2, 3):
        tok_right(m).wait_recv()
    compute(4)
    compute(5)
    fin_hop(4)
    C(7)
    fo_hop()
    sib_in(6).wait_recv()
    sib_in(7).wait_recv()
    for pair in ((0, 1), (2, 3), (4, 5)):
        for i in pair:
            tok_fwd(i).wait_recv()
        if pair[0] == 4:
            for k in (6, 7):
                product(k, pl.ds(mem + small, mem))
        for i in pair:
            m, first, n = pieces[i]
            if pair[0] < 4:
                for k in (6, 7):
                    product(k, pl.ds(first, n))
            epilogue(m, first, n)
        if pair[0] == 0:
            fin_up_in(4).wait_recv()
            fin_dn_in(4).wait_recv()
            fin_sib().start()

    def g_x(k):
        pop, tp = xy_peer(k)
        return rc(FX.at[0], FX.at[k], s_gx, gx, pop, tp)

    for k in range(1, 16):
        g_x(k).start()
    arrived(FX.at[1:16], gx)
    plane = FX[0]
    for k in range(1, 16):
        plane = plane + FX[k]
    FZ[z * 2 + c] = plane

    def g_z(k):
        ref = FZ.at[z * 2 + c]
        return rc(ref, ref, s_gz, gz, zc_peer(k), x)

    for k in range(1, 16):
        g_z(k).start()
    def left(ref, sem):
        rc(ref, ref, sem, fnc, p, x).wait_send()

    @pl.when(off != 0)
    def _():
        send_a.wait_send()

    left(FIN.at[0, 0:3, 0], s_fx)
    left(FIN.at[0, 0:3, 0], s_fny)
    left(T.at[0:2], s_tok)
    left(T.at[0], s_tf)

    @pl.when((rz >= 1) & (rz <= 3))
    def _():
        left(W.at[0, 0, 0:8 * sr], s_z.at[0])

    @pl.when(rz == 0)
    def _():
        left(W.at[0, 0, 0:4 * sr], s_z.at[0])

    @pl.when((rz == 0) | (rz >= 6))
    def _():
        left(W.at[0, 0, 0:8 * sr], s_z.at[1])

    @pl.when(rz == 1)
    def _():
        left(W.at[0, 0, 0:4 * sr], s_z.at[1])

    for d in range(2):
        left(W.at[0, 0, 0:8 * sr], s_y.at[d])
        left(W.at[0, 0, 0:4 * sr], s_f.at[d])
    left(W.at[0:2, :, 0:8 * sr], s_d2)
    left(FIN.at[0:7, :, 0], s_fnz)
    fin_sib().wait_send()
    left(FOS.at[0:7], s_foy)
    left(FO3.at[0:7], s_foz)
    arrived(FO3.at[0:7], foz)
    fin_sib_in().wait_recv()
    left(FX.at[0:15], s_gx)
    left(FZ.at[0:15], s_gz)
    arrived(FZ.at[0:15], gz)

    tiles = FZ[...].reshape(8, 2, 8, 128)
    grid = (tiles[:, 0] + tiles[:, 1]).reshape(64, 128)
    mean = jnp.sum(grid) / 256.0
    wide = jnp.broadcast_to(grid[:, None, :], (64, 16, 128)).reshape(1024, 128)
    rr = lax.broadcasted_iota(jnp.int32, (1024, 128), 0)
    cc = lax.broadcasted_iota(jnp.int32, (1024, 128), 1)
    mine = jnp.where(cc == lax.rem(rr, 16) // 4, wide, 0.0)
    centered = jnp.sum(mine, axis=1, keepdims=True) - mean
    scaled = (centered * FO3[...].reshape(1024, 128).astype(F32)).astype(BF16)
    delta = lax.dot_general(scaled, FIN[...].reshape(1024, kw), (((0,), (0,)), ((), ())),
                            preferred_element_type=F32)
    neww[...] = (WL[...].astype(F32) + step_scale / math.sqrt(1024.0) * delta[0:sr]).astype(BF16)


def local(tokens, target, weight, factor_out, factor_in):
    rows, kw = tokens.shape
    sr = weight.shape[0]
    half = 8 * sr
    width = factor_out.shape[2]
    any_spec = pl.BlockSpec(memory_space=pltpu.HBM)
    vm = pl.BlockSpec(memory_space=pltpu.VMEM)
    D = pltpu.SemaphoreType.DMA
    scratch = [
        pltpu.VMEM(factor_out.shape, BF16),
        pltpu.VMEM(factor_in.shape, BF16),
        pltpu.VMEM((4, rows, kw), BF16),
        pltpu.VMEM((4, 2, half + 16, kw), BF16),
        pltpu.VMEM((8, 4, 2, 16, kw), BF16),
        pltpu.VMEM((rows, kw), BF16),
        pltpu.VMEM((sr, kw), BF16),
        pltpu.VMEM((2, rows, half + 16), F32),
        pltpu.VMEM((16, width), F32),
        pltpu.VMEM((8, 8, 16, 128), BF16),
        pltpu.VMEM((8, 8, 16, 128), BF16),
        pltpu.VMEM((8, 8, 16, 128), BF16),
        pltpu.VMEM((16, kw), BF16),
        pltpu.VMEM((16, 8, 128), F32),
        pltpu.VMEM((16, 8, 128), F32),
        D((6,)), D((4,)), D((4,)), D((6,)), D((4,)), D((16,)), D((16,)), D((8,)), D((8,)),
        D(()), D(()), D((5,)), D((5,)), D(()), D(()), D(()), D(()), D(()),
        D(()), D(()), D(()), D((2,)), D((2,)), D((2,)), D(()), D(()), D(()), D(()), D(()),
        D(()), D(()), D(()), D(()),
    ]
    return pl.pallas_call(
        kernel,
        out_shape=(pltpu.VMEM((rows, kw), BF16), pltpu.VMEM((sr, kw), BF16)),
        in_specs=[any_spec] * 5,
        out_specs=(vm, vm),
        scratch_shapes=scratch,
        compiler_params=pltpu.CompilerParams(
            collective_id=0, has_side_effects=True, vmem_limit_bytes=56 * 1024 * 1024),
    )(tokens, target, weight, factor_out, factor_in)


def solution(mesh):
    from jax.sharding import PartitionSpec as P

    in_specs = (
        P("pop", "tp"),
        P("pop", "tp"),
        P("pop", "tp"),
        P("pop", None, None),
        P("pop", None, "tp"),
    )
    out_specs = (P("pop", "tp"), P("pop", "tp"))
    return jax.shard_map(local, mesh=mesh, in_specs=in_specs, out_specs=out_specs, check_vma=False)
```

```python
import math

import jax
import jax.numpy as jnp
from jax import lax
from jax.experimental import pallas as pl
from jax.experimental.pallas import tpu as pltpu

noise_scale = 0.25
step_scale = 10.0

F32 = jnp.float32
BF16 = jnp.bfloat16
NX, NY, NZ = 4, 4, 8
NSTEP = 8


def kernel(tok, tgt, wt, fo_hbm, fin_hbm, out, neww,
           fo, fin, T, W, FIN, TG, WL, ACC, S32, FOS, FO2, FO3, FP, FX, FZ, STG,
           loc, tr, tl, tf, wa, wz, yin, ff, d2, fxs, fny, fnu, fnd, fnc,
           foy, foz, gx, gz, st, s_rl,
           s_tok, s_tf, s_wa, s_z, s_y, s_f, s_d2, s_fx, s_fny, s_fnz, s_fnc, s_foy, s_foz, s_gx, s_gz):
    p = lax.axis_index("pop")
    x = lax.axis_index("tp")
    z = p // 8
    e = p % 8
    y = e // 2
    c = e % 2
    rows, kw = tok.shape
    mem = rows // 4
    sr = wt.shape[0]
    half = 8 * sr
    rank16 = 16
    width_in = kw * NX
    width_out = width_in

    def pop_of(zz, ee):
        return lax.rem(zz, 8) * 8 + lax.rem(ee, 8)

    def rc(src, dst, ss, rs, pop, tp):
        return pltpu.make_async_remote_copy(
            src_ref=src, dst_ref=dst, send_sem=ss, recv_sem=rs,
            device_id={"pop": pop, "tp": tp}, device_id_type=pl.DeviceIdType.MESH)

    xr = lax.rem(x + 1, 4)
    xl = lax.rem(x + 3, 4)
    zu = pop_of(z + 1, e)
    zd = pop_of(z + 7, e)
    yup = z * 8 + lax.rem(y + 1, 4) * 2 + c
    ydn = z * 8 + lax.rem(y + 3, 4) * 2 + c
    sib = z * 8 + y * 2 + (1 - c)

    l_wl = pltpu.make_async_copy(wt, WL, loc.at[0])
    l_t0 = pltpu.make_async_copy(tok, T.at[0], loc.at[1])
    l_tg = pltpu.make_async_copy(tgt, TG, loc.at[2])
    l_fi = pltpu.make_async_copy(fin_hbm, fin, loc.at[4])
    l_fo = pltpu.make_async_copy(fo_hbm, fo, loc.at[5])
    l_fi.start()
    l_fo.start()
    l_wl.start()
    l_t0.start()
    l_tg.start()

    bar = pltpu.get_barrier_semaphore()
    def xy_peer(k):
        return z * 8 + lax.rem(y + k // 4, 4) * 2 + c, lax.rem(x + k % 4, 4)

    def zc_peer(k):
        return lax.rem(z + k % 8, 8) * 8 + y * 2 + lax.rem(c + k // 8, 2)

    partners = [xy_peer(k) for k in range(1, 16)] + [(zc_peer(k), x) for k in range(1, 16)]
    partners += [(z * 8 + lax.rem(y + k, 4) * 2 + 1 - c, x) for k in range(1, 4)]
    for pop, tp in partners:
        pl.semaphore_signal(bar, inc=1, device_id={"pop": pop, "tp": tp},
                            device_id_type=pl.DeviceIdType.MESH)
    pl.semaphore_wait(bar, 33)

    zt = z // 2
    r_own = lax.rem(z, 2)
    off = lax.rem(x - zt + 4, 4)
    slot = off + off // 2 - 2 * (off // 3)
    shard = pl.ds(pl.multiple_of(e * sr, 16), sr)
    send_a = rc(wt, W.at[slot, r_own, shard], s_wa, wa.at[slot], p, zt)
    copy_a = pltpu.make_async_copy(wt, W.at[0, r_own, shard], loc.at[3])

    @pl.when(off == 0)
    def _():
        copy_a.start()

    def half_of(h):
        return pl.ds(h * (kw // 2), kw // 2)

    def split_a(h):
        return rc(wt.at[:, half_of(h)], STG, s_wa, st, p, (xl, xr)[h])

    def relay(h):
        return rc(STG, W.at[3, r_own, shard, half_of(h)], s_rl, wa.at[3], p, (xl, xr)[h])

    @pl.when((off == 1) | (off == 3))
    def _():
        send_a.start()

    @pl.when(off == 2)
    def _():
        split_a(0).start()
        split_a(1).start()

    xslot = {1: 2, 2: 3, 3: 1}
    def chunk(m):
        return pl.ds(m * mem, mem)

    def tok_right(m):
        return rc(tok.at[chunk(m)], T.at[2, chunk(m)], s_tok, tr.at[m], p, xr)

    def tok_left(m):
        return rc(tok.at[chunk(m)], T.at[1, chunk(m)], s_tok, tl.at[m], p, xl)

    small = mem // 2
    pieces = ((0, 0, mem), (3, 3 * mem, mem), (1, mem, small), (2, 2 * mem + small, small),
              (1, mem + small, small), (2, 2 * mem, small))

    def tok_fwd(i):
        m, first, n = pieces[i]
        rws = pl.ds(first, n)
        side, to = (1, xl) if m >= 2 else (2, xr)
        return rc(T.at[side, rws], T.at[3, rws], s_tf, tf.at[i], p, to)

    for m in range(4):
        tok_right(m).start()
        tok_left(3 - m).start()
        if m == 0:
            for h in range(2):
                @pl.when(off == 1 + 2 * h)
                def _():
                    rc(STG, STG, s_rl, st, p, x).wait_recv()
                    relay(h).start()

    l_fi.wait()
    for i in range(4):
        S32[4 * i:4 * i + 4, 0:kw] = fin[i].astype(F32)
    fin16 = S32[:, 0:kw].astype(BF16)
    FP[...] = fin16
    FIN[z, y, c] = fin16
    W[0, 0, half:half + rank16] = fin16
    def fin_y(k):
        return rc(FP, FIN.at[z, y, c], s_fny, fny,
                  z * 8 + lax.rem(y + k, 4) * 2 + c, x)


    def fo_y(k):
        ee = lax.rem(e + k, 8)
        return rc(FOS.at[ee], FO2.at[e], s_foy, foy, z * 8 + ee, x)

    def fo_cut():
        l_fo.wait()
        for i in range(4):
            S32[4 * i:4 * i + 4, :] = fo[i].astype(F32)
        grp = 8 * sr
        sel_row = lax.broadcasted_iota(jnp.int32, (grp, 1024), 0)
        sel_col = lax.broadcasted_iota(jnp.int32, (grp, 1024), 1)
        lane = lax.rem(sel_col, 128)
        want = (sel_col // 128) * sr + lane
        sel = jnp.where((sel_row == want) & (lane < sr), 1.0, 0.0).astype(BF16)
        for g in range(8):
            cut = jnp.dot(S32[:, g * grp:(g + 1) * grp].astype(BF16), sel,
                          preferred_element_type=F32).astype(BF16)
            for d in range(8):
                FOS[d, g] = cut[:, d * 128:(d + 1) * 128]
        FO2[e] = FOS[e]
        for k in range(1, 8):
            fo_y(k).start()

    def fo_z(k):
        zz = lax.rem(z + k, 8)
        return rc(FO2.at[:, zz], FO3.at[z], s_foz, foz, zz * 8 + e, x)

    l_wl.wait()
    l_t0.wait()
    l_tg.wait()

    rz = lax.rem(z + 8 - 2 * x, 8)

    def shard_at(s, yy, h=None):
        q = lax.rem(yy, 4) * 2 + c
        rws = pl.ds(pl.multiple_of(q * sr, 16), sr)
        if h is None:
            return W.at[s // 2, s % 2, rws]
        return W.at[s // 2, s % 2, rws, pl.ds(h * (kw // 2), kw // 2)]

    def piece(s, yy, h, ss, rs, pop):
        return rc(shard_at(s, yy, h), shard_at(s, yy, h), ss, rs, pop, x)

    def z_send(s, h, d):
        return piece(s, y, h, s_z.at[d], wz.at[2 * s + h], (zu, zd)[d])

    def z_in(s, h):
        return piece(s, y, h, s_z.at[0], wz.at[2 * s + h], p)

    def y_send(s, h, d):
        return piece(s, y, h, s_y.at[d], yin.at[2 * s + h], (yup, ydn)[d])

    def f_send(s, d):
        return piece(s, y + (3, 1)[d], d, s_f.at[d], ff.at[s], (yup, ydn)[d])

    def arrived(ref, sem):
        rc(ref, ref, s_wa, sem, p, x).wait_recv()

    def pass_on(s, k):
        return rc(shard_at(s, y + k), shard_at(s, y + k), s_d2, d2.at[s], sib, x)

    def sib_in(s):
        whole = W.at[s // 2, s % 2, 0:4 * sr]
        return rc(whole, whole, s_d2, d2.at[s], p, x)

    def z_pred(s, d):
        if d == 0:
            return rz <= 3 if s % 2 == 0 else (rz >= 1) & (rz <= 3)
        return (rz == 0) | (rz >= 6) if s % 2 == 0 else (rz <= 1) | (rz >= 6)

    def stage_a(s, h):
        j, r = s // 2, s % 2

        if h == 0:
            @pl.when(rz == r)
            def _():
                if j == 0:
                    copy_a.wait()
                else:
                    rc(shard_at(s, y), shard_at(s, y), s_wa, wa.at[j], p, x).wait_recv()

        @pl.when(rz != r)
        def _():
            z_in(s, h).wait_recv()

        for d in range(2):
            @pl.when(z_pred(s, d))
            def _():
                z_send(s, h, d).start()

        for d in range(2):
            y_send(s, h, d).start()
        if h == 1:
            pass_on(s, 0).start()

    def stage_b(s, h):
        arrived(W.at[0, 0, 0:2 * sr, 0:kw // 2], yin.at[2 * s + h])
        f_send(s, h).start()
        if h == 1:
            pass_on(s, 3).start()
            pass_on(s, 1).start()

    def stage_c(s):
        arrived(shard_at(s, y + 2), ff.at[s])
        pass_on(s, 2).start()

    def product(s, rws):
        j, r = s // 2, s % 2
        prod = lax.dot_general(T[j, rws], W[j, r], (((1,), (1,)), ((), ())),
                               preferred_element_type=F32)
        if j == 0:
            ACC[r, rws] = prod
        else:
            ACC[r, rws] += prod

    def compute(s):
        sib_in(s).wait_recv()
        blk = rows // 2

        def body(i, _):
            product(s, pl.ds(pl.multiple_of(i * blk, blk), blk))
            return 0

        lax.fori_loop(0, 2, body, 0)

    def fin_block(zz, lo, n):
        return FIN.at[lax.rem(zz, 8), lo:lo + n, c]

    def fin_up(h):
        lo, n = (0, 4) if h < 4 else (0, 2)
        ref = fin_block(z + 9 - h, lo, n)
        return rc(ref, ref, s_fnz, fnu.at[h], zu, x)

    def fin_up_in(h):
        lo, n = (0, 4) if h < 4 else (0, 2)
        ref = fin_block(z + 8 - h, lo, n)
        return rc(ref, ref, s_fnz, fnu.at[h], p, x)

    def fin_dn(h):
        lo, n = (0, 4) if h < 4 else (2, 2)
        ref = fin_block(z + h - 1, lo, n)
        return rc(ref, ref, s_fnz, fnd.at[h], zd, x)

    def fin_dn_in(h):
        lo, n = (0, 4) if h < 4 else (2, 2)
        ref = fin_block(z + h, lo, n)
        return rc(ref, ref, s_fnz, fnd.at[h], p, x)

    def fin_sib():
        ref = FIN.at[:, :, c]
        return rc(ref, ref, s_fnc, fnc, sib, x)

    def fin_sib_in():
        ref = FIN.at[:, :, 1 - c]
        return rc(ref, ref, s_fnc, fnc, p, x)

    base_factor = 1.0 / math.sqrt(width_in)
    low_factor = noise_scale / math.sqrt(4 * width_in)
    lanes = lax.broadcasted_iota(jnp.int32, (8, 128), 1)
    sub = lax.broadcasted_iota(jnp.int32, (8, 128), 0)

    def epilogue(m, first, n):
        rws = slice(first, first + n)
        codes = ACC[0, rws, half:half + rank16]
        col = lax.broadcasted_iota(jnp.int32, (n, rank16), 1)
        codes = jnp.where(col // 4 == m, codes, 0.0)
        hi = codes.astype(BF16)
        lo = (codes - hi.astype(F32)).astype(BF16)
        for r in range(2):
            cols = slice(r * half, (r + 1) * half)
            outer = S32[:, pl.ds(pl.multiple_of(x * kw + r * half, 128), half)].astype(BF16)
            low = jnp.dot(hi, outer, preferred_element_type=F32) + jnp.dot(
                lo, outer, preferred_element_type=F32)
            full = ACC[r, rws, 0:half] * base_factor + low * low_factor
            out[rws, cols] = full.astype(BF16)
            part = jnp.sum(full * TG[rws, cols].astype(F32)) / (mem * math.sqrt(width_out))
            FX[0] += jnp.where((sub == e) & (lanes == m), part, 0.0)

    FX[0] = jnp.zeros((8, 128), F32)

    zone = (rz <= 1, (rz == 2) | (rz == 7), (rz >= 3) & (rz <= 6))

    def fwd(which, pair):
        @pl.when(zone[which])
        def _():
            for m in ((0, 3), (1, 2))[pair]:
                (tok_left if m >= 2 else tok_right)(m).wait_recv()
            for i in ((0, 1), (2, 3, 4, 5))[pair]:
                tok_fwd(i).start()

    def fin_hop(h):
        if h == 1:
            arrived(FIN.at[z, 0:3, c], fny)
        else:
            fin_up_in(h - 1).wait_recv()
            fin_dn_in(h - 1).wait_recv()
        fin_up(h).start()
        fin_dn(h).start()

    def tokens_in():
        arrived(W.at[0, 0, 0:3 * rank16], fxs)
        for m in (0, 1):
            tok_left(m).wait_recv()

    def fo_hop():
        arrived(FO2.at[0:7], foy)
        for k in range(1, 8):
            fo_z(k).start()
        FO3[z] = FO2[:, z]

    A, B, C = stage_a, stage_b, stage_c
    A(0, 0)
    A(0, 1)
    for k in range(1, 4):
        rc(FP, W.at[xslot[k], 0, half:half + rank16], s_fx, fxs, p, lax.rem(x + k, 4)).start()
    for k in range(1, 4):
        fin_y(k).start()
    fo_cut()
    A(1, 0)
    B(0, 0)
    A(1, 1)
    B(0, 1)
    fwd(2, 0)
    A(2, 0)
    fin_hop(1)
    B(1, 0)
    A(2, 1)
    C(0)
    B(1, 1)
    A(3, 0)
    fwd(1, 0)
    A(3, 1)
    B(2, 0)
    C(1)
    A(4, 0)
    B(2, 1)
    fwd(2, 1)
    A(4, 1)
    B(3, 0)
    fwd(0, 0)
    A(5, 0)
    C(2)
    fin_hop(2)
    B(3, 1)
    A(5, 1)
    A(6, 0)
    B(4, 0)
    C(3)
    fwd(1, 1)
    A(6, 1)
    compute(0)
    B(4, 1)
    A(7, 0)
    compute(1)
    B(5, 0)
    A(7, 1)
    C(4)
    fwd(0, 1)
    B(5, 1)
    fin_hop(3)
    B(6, 0)
    C(5)
    B(6, 1)
    tokens_in()
    compute(2)
    B(7, 0)
    C(6)
    compute(3)
    B(7, 1)
    for m in (2, 3):
        tok_right(m).wait_recv()
    compute(4)
    compute(5)
    fin_hop(4)
    C(7)
    fo_hop()
    sib_in(6).wait_recv()
    sib_in(7).wait_recv()
    for pair in ((0, 1), (2, 3), (4, 5)):
        for i in pair:
            tok_fwd(i).wait_recv()
        if pair[0] == 4:
            for k in (6, 7):
                product(k, pl.ds(mem + small, mem))
        for i in pair:
            m, first, n = pieces[i]
            if pair[0] < 4:
                for k in (6, 7):
                    product(k, pl.ds(first, n))
            epilogue(m, first, n)
        if pair[0] == 0:
            fin_up_in(4).wait_recv()
            fin_dn_in(4).wait_recv()
            fin_sib().start()

    def g_x(k):
        pop, tp = xy_peer(k)
        return rc(FX.at[0], FX.at[k], s_gx, gx, pop, tp)

    for k in range(1, 16):
        g_x(k).start()
    arrived(FX.at[1:16], gx)
    plane = FX[0]
    for k in range(1, 16):
        plane = plane + FX[k]
    FZ[z * 2 + c] = plane

    def g_z(k):
        ref = FZ.at[z * 2 + c]
        return rc(ref, ref, s_gz, gz, zc_peer(k), x)

    for k in range(1, 16):
        g_z(k).start()
    def left(ref, sem):
        rc(ref, ref, sem, fnc, p, x).wait_send()

    @pl.when(off != 0)
    def _():
        send_a.wait_send()

    for h in range(2):
        @pl.when(off == 1 + 2 * h)
        def _():
            relay(h).wait_send()

    left(FIN.at[0, 0:3, 0], s_fx)
    left(FIN.at[0, 0:3, 0], s_fny)
    left(T.at[0:2], s_tok)
    left(T.at[0], s_tf)

    @pl.when((rz >= 1) & (rz <= 3))
    def _():
        left(W.at[0, 0, 0:8 * sr], s_z.at[0])

    @pl.when(rz == 0)
    def _():
        left(W.at[0, 0, 0:4 * sr], s_z.at[0])

    @pl.when((rz == 0) | (rz >= 6))
    def _():
        left(W.at[0, 0, 0:8 * sr], s_z.at[1])

    @pl.when(rz == 1)
    def _():
        left(W.at[0, 0, 0:4 * sr], s_z.at[1])

    for d in range(2):
        left(W.at[0, 0, 0:8 * sr], s_y.at[d])
        left(W.at[0, 0, 0:4 * sr], s_f.at[d])
    left(W.at[0:2, :, 0:8 * sr], s_d2)
    left(FIN.at[0:7, :, 0], s_fnz)
    fin_sib().wait_send()
    left(FOS.at[0:7], s_foy)
    left(FO3.at[0:7], s_foz)
    arrived(FO3.at[0:7], foz)
    fin_sib_in().wait_recv()
    left(FX.at[0:15], s_gx)
    left(FZ.at[0:15], s_gz)
    arrived(FZ.at[0:15], gz)

    tiles = FZ[...].reshape(8, 2, 8, 128)
    grid = (tiles[:, 0] + tiles[:, 1]).reshape(64, 128)
    mean = jnp.sum(grid) / 256.0
    wide = jnp.broadcast_to(grid[:, None, :], (64, 16, 128)).reshape(1024, 128)
    rr = lax.broadcasted_iota(jnp.int32, (1024, 128), 0)
    cc = lax.broadcasted_iota(jnp.int32, (1024, 128), 1)
    mine = jnp.where(cc == lax.rem(rr, 16) // 4, wide, 0.0)
    centered = jnp.sum(mine, axis=1, keepdims=True) - mean
    scaled = (centered * FO3[...].reshape(1024, 128).astype(F32)).astype(BF16)
    delta = lax.dot_general(scaled, FIN[...].reshape(1024, kw), (((0,), (0,)), ((), ())),
                            preferred_element_type=F32)
    neww[...] = (WL[...].astype(F32) + step_scale / math.sqrt(1024.0) * delta[0:sr]).astype(BF16)


def local(tokens, target, weight, factor_out, factor_in):
    rows, kw = tokens.shape
    sr = weight.shape[0]
    half = 8 * sr
    width = factor_out.shape[2]
    any_spec = pl.BlockSpec(memory_space=pltpu.HBM)
    vm = pl.BlockSpec(memory_space=pltpu.VMEM)
    D = pltpu.SemaphoreType.DMA
    scratch = [
        pltpu.VMEM(factor_out.shape, BF16),
        pltpu.VMEM(factor_in.shape, BF16),
        pltpu.VMEM((4, rows, kw), BF16),
        pltpu.VMEM((4, 2, half + 16, kw), BF16),
        pltpu.VMEM((8, 4, 2, 16, kw), BF16),
        pltpu.VMEM((rows, kw), BF16),
        pltpu.VMEM((sr, kw), BF16),
        pltpu.VMEM((2, rows, half + 16), F32),
        pltpu.VMEM((16, width), F32),
        pltpu.VMEM((8, 8, 16, 128), BF16),
        pltpu.VMEM((8, 8, 16, 128), BF16),
        pltpu.VMEM((8, 8, 16, 128), BF16),
        pltpu.VMEM((16, kw), BF16),
        pltpu.VMEM((16, 8, 128), F32),
        pltpu.VMEM((16, 8, 128), F32),
        pltpu.VMEM((sr, kw // 2), BF16),
        D((6,)), D((4,)), D((4,)), D((6,)), D((4,)), D((16,)), D((16,)), D((8,)), D((8,)),
        D(()), D(()), D((5,)), D((5,)), D(()), D(()), D(()), D(()), D(()), D(()), D(()),
        D(()), D(()), D(()), D((2,)), D((2,)), D((2,)), D(()), D(()), D(()), D(()), D(()),
        D(()), D(()), D(()), D(()),
    ]
    return pl.pallas_call(
        kernel,
        out_shape=(pltpu.VMEM((rows, kw), BF16), pltpu.VMEM((sr, kw), BF16)),
        in_specs=[any_spec] * 5,
        out_specs=(vm, vm),
        scratch_shapes=scratch,
        compiler_params=pltpu.CompilerParams(
            collective_id=0, has_side_effects=True, vmem_limit_bytes=56 * 1024 * 1024),
    )(tokens, target, weight, factor_out, factor_in)


def solution(mesh):
    from jax.sharding import PartitionSpec as P

    in_specs = (
        P("pop", "tp"),
        P("pop", "tp"),
        P("pop", "tp"),
        P("pop", None, None),
        P("pop", None, "tp"),
    )
    out_specs = (P("pop", "tp"), P("pop", "tp"))
    return jax.shard_map(local, mesh=mesh, in_specs=in_specs, out_specs=out_specs, check_vma=False)
```

```python
import math

import jax
import jax.numpy as jnp
from jax import lax
from jax.experimental import pallas as pl
from jax.experimental.pallas import tpu as pltpu

noise_scale = 0.25
step_scale = 10.0

F32 = jnp.float32
BF16 = jnp.bfloat16
NX, NY, NZ = 4, 4, 8
NSTEP = 8


def kernel(tok, tgt, wt, fo_hbm, fin_hbm, out, neww,
           fo, fin, T, W, FIN, TG, WL, ACC, S32, FOS, FO2, FO3, FP, FX, FZ, STG, FIT,
           loc, tr, tl, tf, wa, wz, yin, ff, d2, fxs, fny, fnu, fnd, fnc,
           foy, foz, gx, gz, st, s_rl,
           s_tok, s_tf, s_wa, s_z, s_y, s_f, s_d2, s_fx, s_fny, s_fnz, s_fnc, s_foy, s_foz, s_gx, s_gz):
    p = lax.axis_index("pop")
    x = lax.axis_index("tp")
    z = p // 8
    e = p % 8
    y = e // 2
    c = e % 2
    rows, kw = tok.shape
    mem = rows // 4
    sr = wt.shape[0]
    half = 8 * sr
    rank16 = 16
    width_in = kw * NX
    width_out = width_in

    def pop_of(zz, ee):
        return lax.rem(zz, 8) * 8 + lax.rem(ee, 8)

    def rc(src, dst, ss, rs, pop, tp):
        return pltpu.make_async_remote_copy(
            src_ref=src, dst_ref=dst, send_sem=ss, recv_sem=rs,
            device_id={"pop": pop, "tp": tp}, device_id_type=pl.DeviceIdType.MESH)

    xr = lax.rem(x + 1, 4)
    xl = lax.rem(x + 3, 4)
    zu = pop_of(z + 1, e)
    zd = pop_of(z + 7, e)
    yup = z * 8 + lax.rem(y + 1, 4) * 2 + c
    ydn = z * 8 + lax.rem(y + 3, 4) * 2 + c
    sib = z * 8 + y * 2 + (1 - c)

    l_wl = pltpu.make_async_copy(wt, WL, loc.at[0])
    l_t0 = pltpu.make_async_copy(tok, T.at[0], loc.at[1])
    l_tg = pltpu.make_async_copy(tgt, TG, loc.at[2])
    l_fi = pltpu.make_async_copy(fin_hbm, fin, loc.at[4])
    l_fo = pltpu.make_async_copy(fo_hbm, fo, loc.at[5])
    l_fi.start()
    l_fo.start()
    l_wl.start()
    l_t0.start()
    l_tg.start()

    bar = pltpu.get_barrier_semaphore()
    def xy_peer(k):
        return z * 8 + lax.rem(y + k // 4, 4) * 2 + c, lax.rem(x + k % 4, 4)

    def zc_peer(k):
        return lax.rem(z + k % 8, 8) * 8 + y * 2 + lax.rem(c + k // 8, 2)

    partners = [xy_peer(k) for k in range(1, 16)] + [(zc_peer(k), x) for k in range(1, 16)]
    partners += [(z * 8 + lax.rem(y + k, 4) * 2 + 1 - c, x) for k in range(1, 4)]
    for pop, tp in partners:
        pl.semaphore_signal(bar, inc=1, device_id={"pop": pop, "tp": tp},
                            device_id_type=pl.DeviceIdType.MESH)
    pl.semaphore_wait(bar, 33)

    zt = z // 2
    r_own = lax.rem(z, 2)
    off = lax.rem(x - zt + 4, 4)
    slot = off + off // 2 - 2 * (off // 3)
    shard = pl.ds(pl.multiple_of(e * sr, 16), sr)
    send_a = rc(wt, W.at[slot, r_own, shard], s_wa, wa.at[slot], p, zt)
    copy_a = pltpu.make_async_copy(wt, W.at[0, r_own, shard], loc.at[3])

    @pl.when(off == 0)
    def _():
        copy_a.start()

    def half_of(h):
        return pl.ds(h * (kw // 2), kw // 2)

    def split_a(h):
        return rc(wt.at[:, half_of(h)], STG, s_wa, st, p, (xl, xr)[h])

    def relay(h):
        return rc(STG, W.at[3, r_own, shard, half_of(h)], s_rl, wa.at[3], p, (xl, xr)[h])

    @pl.when((off == 1) | (off == 3))
    def _():
        send_a.start()

    @pl.when(off == 2)
    def _():
        split_a(0).start()
        split_a(1).start()

    xslot = {1: 2, 2: 3, 3: 1}
    def chunk(m):
        return pl.ds(m * mem, mem)

    def tok_right(m):
        return rc(tok.at[chunk(m)], T.at[2, chunk(m)], s_tok, tr.at[m], p, xr)

    def tok_left(m):
        return rc(tok.at[chunk(m)], T.at[1, chunk(m)], s_tok, tl.at[m], p, xl)

    small = mem // 4
    pieces = ((0, 0, mem), (3, 3 * mem, mem), (1, mem, mem - small), (2, 2 * mem + small, mem - small),
              (1, 2 * mem - small, small), (2, 2 * mem, small))

    def tok_fwd(i):
        m, first, n = pieces[i]
        rws = pl.ds(first, n)
        side, to = (1, xl) if m >= 2 else (2, xr)
        return rc(T.at[side, rws], T.at[3, rws], s_tf, tf.at[i], p, to)

    for m in range(4):
        tok_right(m).start()
        tok_left(3 - m).start()
        if m == 0:
            for h in range(2):
                @pl.when(off == 1 + 2 * h)
                def _():
                    rc(STG, STG, s_rl, st, p, x).wait_recv()
                    relay(h).start()

    l_fi.wait()
    for i in range(4):
        S32[4 * i:4 * i + 4, 0:kw] = fin[i].astype(F32)
    fin16 = S32[:, 0:kw].astype(BF16)
    FP[...] = fin16
    FIN[z, y, c] = fin16
    W[0, 0, half:half + rank16] = fin16
    def fin_y(k):
        return rc(FP, FIN.at[z, y, c], s_fny, fny,
                  z * 8 + lax.rem(y + k, 4) * 2 + c, x)


    def fo_y(k):
        ee = lax.rem(e + k, 8)
        return rc(FOS.at[ee], FO2.at[e], s_foy, foy, z * 8 + ee, x)

    def fo_cut():
        l_fo.wait()
        for i in range(4):
            S32[4 * i:4 * i + 4, :] = fo[i].astype(F32)
        grp = 8 * sr
        sel_row = lax.broadcasted_iota(jnp.int32, (grp, 1024), 0)
        sel_col = lax.broadcasted_iota(jnp.int32, (grp, 1024), 1)
        lane = lax.rem(sel_col, 128)
        want = (sel_col // 128) * sr + lane
        sel = jnp.where((sel_row == want) & (lane < sr), 1.0, 0.0).astype(BF16)
        for g in range(8):
            cut = jnp.dot(S32[:, g * grp:(g + 1) * grp].astype(BF16), sel,
                          preferred_element_type=F32).astype(BF16)
            for d in range(8):
                FOS[d, g] = cut[:, d * 128:(d + 1) * 128]
        FO2[e] = FOS[e]
        for k in range(1, 8):
            fo_y(k).start()

    def fo_z(k):
        zz = lax.rem(z + k, 8)
        return rc(FO2.at[:, zz], FO3.at[z], s_foz, foz, zz * 8 + e, x)

    l_wl.wait()
    l_t0.wait()
    l_tg.wait()

    rz = lax.rem(z + 8 - 2 * x, 8)

    def shard_at(s, yy, h=None):
        q = lax.rem(yy, 4) * 2 + c
        rws = pl.ds(pl.multiple_of(q * sr, 16), sr)
        if h is None:
            return W.at[s // 2, s % 2, rws]
        return W.at[s // 2, s % 2, rws, pl.ds(h * (kw // 2), kw // 2)]

    def piece(s, yy, h, ss, rs, pop):
        return rc(shard_at(s, yy, h), shard_at(s, yy, h), ss, rs, pop, x)

    def z_send(s, h, d):
        return piece(s, y, h, s_z.at[d], wz.at[2 * s + h], (zu, zd)[d])

    def z_in(s, h):
        return piece(s, y, h, s_z.at[0], wz.at[2 * s + h], p)

    def y_send(s, h, d):
        return piece(s, y, h, s_y.at[d], yin.at[2 * s + h], (yup, ydn)[d])

    def f_send(s, d):
        return piece(s, y + (3, 1)[d], d, s_f.at[d], ff.at[s], (yup, ydn)[d])

    def arrived(ref, sem):
        rc(ref, ref, s_wa, sem, p, x).wait_recv()

    def pass_on(s, k):
        return rc(shard_at(s, y + k), shard_at(s, y + k), s_d2, d2.at[s], sib, x)

    def sib_in(s):
        whole = W.at[s // 2, s % 2, 0:4 * sr]
        return rc(whole, whole, s_d2, d2.at[s], p, x)

    def z_pred(s, d):
        if d == 0:
            return rz <= 3 if s % 2 == 0 else (rz >= 1) & (rz <= 3)
        return (rz == 0) | (rz >= 6) if s % 2 == 0 else (rz <= 1) | (rz >= 6)

    def stage_a(s, h):
        j, r = s // 2, s % 2

        if h == 0:
            @pl.when(rz == r)
            def _():
                if j == 0:
                    copy_a.wait()
                else:
                    rc(shard_at(s, y), shard_at(s, y), s_wa, wa.at[j], p, x).wait_recv()

        @pl.when(rz != r)
        def _():
            z_in(s, h).wait_recv()

        for d in range(2):
            @pl.when(z_pred(s, d))
            def _():
                z_send(s, h, d).start()

        for d in range(2):
            y_send(s, h, d).start()
        if h == 1:
            pass_on(s, 0).start()

    def stage_b(s, h):
        arrived(W.at[0, 0, 0:2 * sr, 0:kw // 2], yin.at[2 * s + h])
        f_send(s, h).start()
        if h == 1:
            pass_on(s, 3).start()
            pass_on(s, 1).start()

    def stage_c(s):
        arrived(shard_at(s, y + 2), ff.at[s])
        pass_on(s, 2).start()

    def product(s, rws):
        j, r = s // 2, s % 2
        prod = lax.dot_general(T[j, rws], W[j, r], (((1,), (1,)), ((), ())),
                               preferred_element_type=F32)
        if j == 0:
            ACC[r, rws] = prod
        else:
            ACC[r, rws] += prod

    def compute(s):
        sib_in(s).wait_recv()
        blk = rows // 2

        def body(i, _):
            product(s, pl.ds(pl.multiple_of(i * blk, blk), blk))
            return 0

        lax.fori_loop(0, 2, body, 0)

    def fin_block(zz, lo, n):
        return FIN.at[lax.rem(zz, 8), lo:lo + n, c]

    def fin_up(h):
        lo, n = (0, 4) if h < 4 else (0, 2)
        ref = fin_block(z + 9 - h, lo, n)
        return rc(ref, ref, s_fnz, fnu.at[h], zu, x)

    def fin_up_in(h):
        lo, n = (0, 4) if h < 4 else (0, 2)
        ref = fin_block(z + 8 - h, lo, n)
        return rc(ref, ref, s_fnz, fnu.at[h], p, x)

    def fin_dn(h):
        lo, n = (0, 4) if h < 4 else (2, 2)
        ref = fin_block(z + h - 1, lo, n)
        return rc(ref, ref, s_fnz, fnd.at[h], zd, x)

    def fin_dn_in(h):
        lo, n = (0, 4) if h < 4 else (2, 2)
        ref = fin_block(z + h, lo, n)
        return rc(ref, ref, s_fnz, fnd.at[h], p, x)

    def fin_sib():
        ref = FIN.at[:, :, c]
        return rc(ref, ref, s_fnc, fnc, sib, x)

    def fin_sib_in():
        ref = FIN.at[:, :, 1 - c]
        return rc(ref, ref, s_fnc, fnc, p, x)

    base_factor = 1.0 / math.sqrt(width_in)
    low_factor = noise_scale / math.sqrt(4 * width_in)
    lanes = lax.broadcasted_iota(jnp.int32, (8, 128), 1)
    sub = lax.broadcasted_iota(jnp.int32, (8, 128), 0)

    def epilogue(m, first, n):
        rws = slice(first, first + n)
        codes = ACC[0, rws, half:half + rank16]
        col = lax.broadcasted_iota(jnp.int32, (n, rank16), 1)
        codes = jnp.where(col // 4 == m, codes, 0.0)
        hi = codes.astype(BF16)
        lo = (codes - hi.astype(F32)).astype(BF16)
        for r in range(2):
            cols = slice(r * half, (r + 1) * half)
            outer = S32[:, pl.ds(pl.multiple_of(x * kw + r * half, 128), half)].astype(BF16)
            low = jnp.dot(hi, outer, preferred_element_type=F32) + jnp.dot(
                lo, outer, preferred_element_type=F32)
            full = ACC[r, rws, 0:half] * base_factor + low * low_factor
            out[rws, cols] = full.astype(BF16)
            part = jnp.sum((full * TG[rws, cols].astype(F32)).reshape(n // 8, 8, half), axis=0)
            for i in range(half // 128):
                FIT[m] += part[:, i * 128:(i + 1) * 128]

    FIT[...] = jnp.zeros(FIT.shape, F32)

    zone = (rz <= 1, (rz == 2) | (rz == 7), (rz >= 3) & (rz <= 6))

    def fwd(which, pair):
        @pl.when(zone[which])
        def _():
            for m in ((0, 3), (1, 2))[pair]:
                (tok_left if m >= 2 else tok_right)(m).wait_recv()
            for i in ((0, 1), (2, 3, 4, 5))[pair]:
                tok_fwd(i).start()

    def fin_hop(h):
        if h == 1:
            arrived(FIN.at[z, 0:3, c], fny)
        else:
            fin_up_in(h - 1).wait_recv()
            fin_dn_in(h - 1).wait_recv()
        fin_up(h).start()
        fin_dn(h).start()

    def tokens_in():
        arrived(W.at[0, 0, 0:3 * rank16], fxs)
        for m in (0, 1):
            tok_left(m).wait_recv()

    def fo_hop():
        arrived(FO2.at[0:7], foy)
        for k in range(1, 8):
            fo_z(k).start()
        FO3[z] = FO2[:, z]

    A, B, C = stage_a, stage_b, stage_c
    A(0, 0)
    A(0, 1)
    for k in range(1, 4):
        rc(FP, W.at[xslot[k], 0, half:half + rank16], s_fx, fxs, p, lax.rem(x + k, 4)).start()
    for k in range(1, 4):
        fin_y(k).start()
    fo_cut()
    A(1, 0)
    B(0, 0)
    A(1, 1)
    B(0, 1)
    fwd(2, 0)
    A(2, 0)
    fin_hop(1)
    B(1, 0)
    A(2, 1)
    C(0)
    B(1, 1)
    A(3, 0)
    fwd(1, 0)
    A(3, 1)
    B(2, 0)
    C(1)
    A(4, 0)
    B(2, 1)
    fwd(2, 1)
    A(4, 1)
    B(3, 0)
    fwd(0, 0)
    A(5, 0)
    C(2)
    fin_hop(2)
    B(3, 1)
    A(5, 1)
    A(6, 0)
    B(4, 0)
    C(3)
    fwd(1, 1)
    A(6, 1)
    compute(0)
    B(4, 1)
    A(7, 0)
    compute(1)
    B(5, 0)
    A(7, 1)
    C(4)
    fwd(0, 1)
    B(5, 1)
    fin_hop(3)
    B(6, 0)
    C(5)
    B(6, 1)
    tokens_in()
    compute(2)
    B(7, 0)
    C(6)
    compute(3)
    B(7, 1)
    for m in (2, 3):
        tok_right(m).wait_recv()
    compute(4)
    compute(5)
    fin_hop(4)
    C(7)
    fo_hop()
    sib_in(6).wait_recv()
    sib_in(7).wait_recv()
    for pair in ((0, 1), (2, 3), (4, 5)):
        for i in pair:
            tok_fwd(i).wait_recv()
        if pair[0] == 4:
            for k in (6, 7):
                product(k, pl.ds(2 * mem - small, 2 * small))
        for i in pair:
            m, first, n = pieces[i]
            if pair[0] < 4:
                for k in (6, 7):
                    product(k, pl.ds(first, n))
            epilogue(m, first, n)
        if pair[0] == 0:
            fin_up_in(4).wait_recv()
            fin_dn_in(4).wait_recv()
            fin_sib().start()

    def g_x(k):
        pop, tp = xy_peer(k)
        return rc(FX.at[0], FX.at[k], s_gx, gx, pop, tp)

    tile = jnp.zeros((8, 128), F32)
    for m in range(4):
        total = jnp.sum(FIT[m]) / (mem * math.sqrt(width_out))
        tile = tile + jnp.where((sub == e) & (lanes == m), total, 0.0)
    FX[0] = tile
    for k in range(1, 16):
        g_x(k).start()
    arrived(FX.at[1:16], gx)
    plane = FX[0]
    for k in range(1, 16):
        plane = plane + FX[k]
    FZ[z * 2 + c] = plane

    def g_z(k):
        ref = FZ.at[z * 2 + c]
        return rc(ref, ref, s_gz, gz, zc_peer(k), x)

    for k in range(1, 16):
        g_z(k).start()
    def left(ref, sem):
        rc(ref, ref, sem, fnc, p, x).wait_send()

    @pl.when(off != 0)
    def _():
        send_a.wait_send()

    for h in range(2):
        @pl.when(off == 1 + 2 * h)
        def _():
            relay(h).wait_send()

    left(FIN.at[0, 0:3, 0], s_fx)
    left(FIN.at[0, 0:3, 0], s_fny)
    left(T.at[0:2], s_tok)
    left(T.at[0], s_tf)

    @pl.when((rz >= 1) & (rz <= 3))
    def _():
        left(W.at[0, 0, 0:8 * sr], s_z.at[0])

    @pl.when(rz == 0)
    def _():
        left(W.at[0, 0, 0:4 * sr], s_z.at[0])

    @pl.when((rz == 0) | (rz >= 6))
    def _():
        left(W.at[0, 0, 0:8 * sr], s_z.at[1])

    @pl.when(rz == 1)
    def _():
        left(W.at[0, 0, 0:4 * sr], s_z.at[1])

    for d in range(2):
        left(W.at[0, 0, 0:8 * sr], s_y.at[d])
        left(W.at[0, 0, 0:4 * sr], s_f.at[d])
    left(W.at[0:2, :, 0:8 * sr], s_d2)
    left(FIN.at[0:7, :, 0], s_fnz)
    fin_sib().wait_send()
    left(FOS.at[0:7], s_foy)
    left(FO3.at[0:7], s_foz)
    arrived(FO3.at[0:7], foz)
    fin_sib_in().wait_recv()
    left(FX.at[0:15], s_gx)
    left(FZ.at[0:15], s_gz)
    arrived(FZ.at[0:15], gz)

    tiles = FZ[...].reshape(8, 2, 8, 128)
    grid = (tiles[:, 0] + tiles[:, 1]).reshape(64, 128)
    mean = jnp.sum(grid) / 256.0
    wide = jnp.broadcast_to(grid[:, None, :], (64, 16, 128)).reshape(1024, 128)
    rr = lax.broadcasted_iota(jnp.int32, (1024, 128), 0)
    cc = lax.broadcasted_iota(jnp.int32, (1024, 128), 1)
    mine = jnp.where(cc == lax.rem(rr, 16) // 4, wide, 0.0)
    centered = jnp.sum(mine, axis=1, keepdims=True) - mean
    scaled = (centered * FO3[...].reshape(1024, 128).astype(F32)).astype(BF16)
    delta = lax.dot_general(scaled, FIN[...].reshape(1024, kw), (((0,), (0,)), ((), ())),
                            preferred_element_type=F32)
    neww[...] = (WL[...].astype(F32) + step_scale / math.sqrt(1024.0) * delta[0:sr]).astype(BF16)


def local(tokens, target, weight, factor_out, factor_in):
    rows, kw = tokens.shape
    sr = weight.shape[0]
    half = 8 * sr
    width = factor_out.shape[2]
    any_spec = pl.BlockSpec(memory_space=pltpu.HBM)
    vm = pl.BlockSpec(memory_space=pltpu.VMEM)
    D = pltpu.SemaphoreType.DMA
    scratch = [
        pltpu.VMEM(factor_out.shape, BF16),
        pltpu.VMEM(factor_in.shape, BF16),
        pltpu.VMEM((4, rows, kw), BF16),
        pltpu.VMEM((4, 2, half + 16, kw), BF16),
        pltpu.VMEM((8, 4, 2, 16, kw), BF16),
        pltpu.VMEM((rows, kw), BF16),
        pltpu.VMEM((sr, kw), BF16),
        pltpu.VMEM((2, rows, half + 16), F32),
        pltpu.VMEM((16, width), F32),
        pltpu.VMEM((8, 8, 16, 128), BF16),
        pltpu.VMEM((8, 8, 16, 128), BF16),
        pltpu.VMEM((8, 8, 16, 128), BF16),
        pltpu.VMEM((16, kw), BF16),
        pltpu.VMEM((16, 8, 128), F32),
        pltpu.VMEM((16, 8, 128), F32),
        pltpu.VMEM((sr, kw // 2), BF16),
        pltpu.VMEM((4, 8, 128), F32),
        D((6,)), D((4,)), D((4,)), D((6,)), D((4,)), D((16,)), D((16,)), D((8,)), D((8,)),
        D(()), D(()), D((5,)), D((5,)), D(()), D(()), D(()), D(()), D(()), D(()), D(()),
        D(()), D(()), D(()), D((2,)), D((2,)), D((2,)), D(()), D(()), D(()), D(()), D(()),
        D(()), D(()), D(()), D(()),
    ]
    return pl.pallas_call(
        kernel,
        out_shape=(pltpu.VMEM((rows, kw), BF16), pltpu.VMEM((sr, kw), BF16)),
        in_specs=[any_spec] * 5,
        out_specs=(vm, vm),
        scratch_shapes=scratch,
        compiler_params=pltpu.CompilerParams(
            collective_id=0, has_side_effects=True, vmem_limit_bytes=56 * 1024 * 1024),
    )(tokens, target, weight, factor_out, factor_in)


def solution(mesh):
    from jax.sharding import PartitionSpec as P

    in_specs = (
        P("pop", "tp"),
        P("pop", "tp"),
        P("pop", "tp"),
        P("pop", None, None),
        P("pop", None, "tp"),
    )
    out_specs = (P("pop", "tp"), P("pop", "tp"))
    return jax.shard_map(local, mesh=mesh, in_specs=in_specs, out_specs=out_specs, check_vma=False)
```
